256 devices in a mesh: gx: 16 (over x_lo, z), gy: 2 (over core), gz: 8 (over y, x_hi).
Axes of the slice: x: 4 (x_hi: 2, x_lo: 2; x = x_hi * 2 + x_lo), y: 4, z: 8, core: 2. Of those that a mesh axis runs over, the one named last changes fastest.
Arguments:
- features: bfloat16 [16, 2, 8, 128, 512], P('gx', 'gy', 'gz'), may hold values from -6 to 6
- fraction: bfloat16 [16, 2, 8, 3, 128], P('gx', 'gy', 'gz'), may hold values from 0 to 0.98828125
- cell_index: int32 [16, 2, 8, 3, 128], P('gx', 'gy', 'gz'), may hold values from 0 to 127, as said below
- species: int32 [16, 2, 8, 128], P('gx', 'gy', 'gz'), may hold values from 0 to 1
- octant_rows: int32 [16, 2, 8, 8, 14], P('gx', 'gy', 'gz'), may hold values from 0 to 127, as said below
- neighbours: int32 [16, 2, 8, 16, 128], P('gx', 'gy', 'gz'), may hold values from 0 to 912, as said below
- radial_in: bfloat16 [2, 8, 64], replicated, may hold values from -2 to 2
- radial_out: bfloat16 [2, 64, 512], replicated, may hold values from -1.5 to 1.5
- mix_weight: bfloat16 [2, 2, 128, 128], replicated, may hold values from -0.5 to 0.5
- readout: bfloat16 [128, 2], replicated, may hold values from -0.125 to 0.125
- species_table: float32 [2, 2], replicated, may hold values from -4 to 4
Outputs:
- new_features: bfloat16 [16, 2, 8, 128, 512], P('gx', 'gy', 'gz')
- site_energy: float32 [16, 2, 8, 128], P('gx', 'gy', 'gz')
- recip_force: float32 [16, 2, 8, 3, 128], P('gx', 'gy', 'gz')
The draws below stay inside these ranges and needn't reach their ends.
Inputs may be any that keep to these rules, and one draw needn't show every extreme that they name: `cell_index`: component x lies below 16, component y below 128, component z below 32. `octant_rows`: each octant's list holds 14 different atoms of the domain. `neighbours`: entries are rows of the domain's table; 912 is an empty slot; an atom never lists itself, and the other entries of a column are different; the cell of a listed row (cell_index plus its shift) lies within 8 cells of the atom's cell.
All inputs are finite; a program needn't handle non-finite values.
Results may differ from the reference program's by a relative error of at most 0.0051.
Values may be sent and summed in bfloat16 or wider, within the bound.
No kernel may reach another device: no remote copies, remote signals or barrier semaphores. Data moves between devices by JAX's collectives and lax.ppermute only.
A program may use at most 64 MiB of HBM per device.

```python
import math
import jax
import jax.numpy as jnp
from jax import lax

C = 128
FEAT = 512
NB = 8
HID = 64
LAYERS = 2
NEIGH = 16
NSPEC = 2
RCUT = 8
ENV = 7
MESH = 256
ATOMS = 128
GHOST = 14
NCAND = 912
BX = 16
BY = 128
BZ = 32
N_GX = 16
N_GY = 2
N_GZ = 8


def outer_cells_drawn():
    found = []
    for first in range(4):
        for second in range(4):
            for third in range(4):
                if 0 < first < 3 and 0 < second < 3 and (0 < third < 3):
                    continue
                found.append((first, second, third))
    return found


def offset_of_drawn(coord):
    return -1 if coord == 0 else 1 if coord == 3 else 0


def source_of_drawn(coord):
    return 1 if coord == 0 else 0 if coord == 3 else coord - 1


def layout(key):
    device_total = N_GX * N_GY * N_GZ
    pair_total = ATOMS // 2
    span_sizes = jnp.array([BX, BY, BZ], jnp.int32).reshape(1, 1, 1, 3, 1)
    half_sizes = span_sizes // 2
    raw_bits = jax.random.randint(jax.random.fold_in(key, 101), (N_GX, N_GY, N_GZ, 3, pair_total), 0, 1 << 24)
    lead_raw = raw_bits % half_sizes
    axis_pick = jax.random.randint(jax.random.fold_in(key, 104), (N_GX, N_GY, N_GZ, 1, pair_total), 1, 3)
    coin_flip = jax.random.randint(jax.random.fold_in(key, 105), (N_GX, N_GY, N_GZ, 1, pair_total), 0, 2)
    step_sign = jnp.where(lead_raw == half_sizes - 1, -1, jnp.where(lead_raw == 0, 1, 2 * coin_flip - 1))
    on_axis = (jnp.arange(3, dtype=jnp.int32).reshape(1, 1, 1, 3, 1) == axis_pick).astype(jnp.int32)
    partner_raw = lead_raw + step_sign * on_axis
    raw_cells = jnp.stack([lead_raw, partner_raw], axis=5).reshape(N_GX, N_GY, N_GZ, 3, ATOMS)
    pair_orders = jax.vmap(lambda subkey: jax.random.permutation(subkey, pair_total))(jax.random.split(jax.random.fold_in(key, 102), device_total))
    pair_orders = pair_orders.astype(jnp.int32).reshape(N_GX, N_GY, N_GZ, pair_total)
    orders = jnp.stack([2 * pair_orders, 2 * pair_orders + 1], axis=4).reshape(N_GX, N_GY, N_GZ, ATOMS)
    octant_of = orders // (ATOMS // 8)
    upper_half = jnp.stack([octant_of // 4, octant_of // 2 % 2, octant_of % 2], axis=3).astype(jnp.int32)
    cells = upper_half * half_sizes + raw_cells
    depth_face = jnp.where(upper_half == 1, span_sizes - 1 - cells, cells)
    nearest = jnp.min(depth_face, axis=3)
    reach_max = BX + BY + BZ
    chosen = []
    for octant in range(8):
        bit_pattern = jnp.array([octant // 4, octant // 2 % 2, octant % 2], jnp.int32).reshape(1, 1, 1, 3, 1)
        inside = jnp.all(upper_half == bit_pattern, axis=3)
        scores = jnp.where(inside, reach_max - nearest, 0) * ATOMS + orders
        chosen.append(lax.top_k(scores, GHOST)[1])
    octants = jnp.stack(chosen, axis=3).astype(jnp.int32)
    pieces = [cells]
    for corner in outer_cells_drawn():
        roll_by = (-offset_of_drawn(corner[0]), -offset_of_drawn(corner[1]), -offset_of_drawn(corner[2]))
        octant = 4 * source_of_drawn(corner[0]) + 2 * source_of_drawn(corner[1]) + source_of_drawn(corner[2])
        source_cells = jnp.roll(cells, roll_by, (0, 1, 2))
        source_rows = jnp.roll(octants[:, :, :, octant], roll_by, (0, 1, 2))
        picker = jnp.broadcast_to(source_rows[:, :, :, None, :], (N_GX, N_GY, N_GZ, 3, GHOST))
        picked = jnp.take_along_axis(source_cells, picker, axis=4)
        shifted = picked + jnp.array([offset_of_drawn(corner[0]) * BX, offset_of_drawn(corner[1]) * BY, offset_of_drawn(corner[2]) * BZ], jnp.int32).reshape(1, 1, 1, 3, 1)
        pieces.append(shifted)
    candidates = jnp.concatenate(pieces, axis=4).reshape(device_total, 3, NCAND)
    shuffles = jax.vmap(lambda subkey: jax.random.permutation(subkey, NCAND))(jax.random.split(jax.random.fold_in(key, 103), device_total)).astype(jnp.int32)
    beyond = RCUT * RCUT + 1

    def pick_slots(inputs):
        located, shuffle = inputs
        differ = located[:, :ATOMS, None] - located[:, None, :]
        distance = jnp.sum(differ * differ, axis=0)
        is_self = jnp.arange(ATOMS, dtype=jnp.int32)[:, None] == jnp.arange(NCAND, dtype=jnp.int32)[None, :]
        measure = jnp.where(is_self, beyond, jnp.minimum(distance, beyond))
        nearest_slots = lax.top_k(-(measure * NCAND + shuffle[None, :]), NEIGH)[1]
        near_value = jnp.take_along_axis(measure, nearest_slots, axis=1)
        return jnp.transpose(jnp.where(near_value <= RCUT * RCUT, nearest_slots, NCAND)).astype(jnp.int32)
    links = lax.map(pick_slots, (candidates, shuffles)).reshape(N_GX, N_GY, N_GZ, NEIGH, ATOMS)
    return (cells.astype(jnp.int32), octants, links)


def draw_cell_index(key, part):
    return layout(key)[0]


def draw_octant_rows(key, part):
    return layout(key)[1]


def draw_neighbours(key, part):
    return layout(key)[2]


def draw_species(key, part):
    leading = jax.random.randint(jax.random.fold_in(key, 201), (N_GX, N_GY, N_GZ, ATOMS // 2), 0, NSPEC)
    partner = (leading + 1) % NSPEC
    return jnp.stack([leading, partner], axis=4).reshape(N_GX, N_GY, N_GZ, ATOMS).astype(jnp.int32)


def draw_species_table(key, part):
    signs = jnp.where(jnp.arange(NSPEC, dtype=jnp.int32) % 2 == 0, 1.0, -1.0).astype(jnp.float32)
    energy = jnp.clip(jax.random.normal(jax.random.fold_in(key, 301), (NSPEC,), jnp.float32), -4.0, 4.0)
    magnitude = jax.random.uniform(jax.random.fold_in(key, 302), (NSPEC,), jnp.float32, 2.5, 3.5)
    return jnp.stack([energy, magnitude * signs], axis=1).astype(jnp.float32)


def block_scale(stream_key, extent, shards, low, largest):
    loudness = 1.0
    for position, shards_of in shards:
        steps = jax.random.uniform(jax.random.fold_in(jax.random.fold_in(stream_key, 6), position), (shards_of,), jnp.float32, low / len(shards), largest / len(shards))
        loudness = loudness * jnp.repeat(jnp.exp(steps), extent[position] // shards_of).reshape((-1,) + (1,) * (len(extent) - 1 - position))
    return loudness


def scatter_about(key, extent, width, most, shards=(), kind=jnp.bfloat16):
    level = block_scale(key, extent, shards, -0.22, 0.18) if shards else 1.0
    drawn = jax.random.normal(key, extent, jnp.float32) * width * level
    return jnp.minimum(jnp.maximum(drawn, -most), most).astype(kind)


def setup_inputs(seed: int = 0) -> dict:
    keys = jax.random.split(jax.random.key(seed), 12)
    return {
        "features": scatter_about(keys[0], (N_GX, N_GY, N_GZ, ATOMS, FEAT), 1.0, 6.0, ((0, 16), (1, 2), (2, 8))),
        "fraction": jnp.clip(0.98828125 * jax.random.uniform(keys[1], (N_GX, N_GY, N_GZ, 3, ATOMS), jnp.float32) ** block_scale(keys[1], (N_GX, N_GY, N_GZ, 3, ATOMS), ((0, 16), (1, 2), (2, 8)), -0.2, 0.2), 0.0, 0.98828125).astype(jnp.bfloat16),
        "cell_index": draw_cell_index(jax.random.fold_in(keys[11], 71), 0),
        "species": draw_species(jax.random.fold_in(keys[11], 71), 0),
        "octant_rows": draw_octant_rows(jax.random.fold_in(keys[11], 71), 0),
        "neighbours": draw_neighbours(jax.random.fold_in(keys[11], 71), 0),
        "radial_in": scatter_about(keys[6], (LAYERS, NB, HID), NB ** -0.5, 2.0),
        "radial_out": scatter_about(keys[7], (LAYERS, HID, FEAT), (HID // 4) ** -0.5, 1.5),
        "mix_weight": scatter_about(keys[8], (LAYERS, 2, C, C), C ** -0.5, 0.5),
        "readout": scatter_about(keys[9], (C, 2), (16 * C) ** -0.5, 0.125),
        "species_table": draw_species_table(jax.random.fold_in(keys[11], 71), 0),
    }


COULOMB = 4.0
EWALD = 0.7

def outer_cells():
    found = []
    for first in range(4):
        for second in range(4):
            for third in range(4):
                if 0 < first < 3 and 0 < second < 3 and (0 < third < 3):
                    continue
                found.append((first, second, third))
    return found

def offset_of(coord):
    return -1 if coord == 0 else 1 if coord == 3 else 0

def source_of(coord):
    return 1 if coord == 0 else 0 if coord == 3 else coord - 1

def spline(fraction_in):
    upper_t = fraction_in
    lower_t = 1.0 - fraction_in
    weights = jnp.stack([lower_t * lower_t * lower_t / 6.0, (3.0 * upper_t * upper_t * upper_t - 6.0 * upper_t * upper_t + 4.0) / 6.0, (-3.0 * upper_t * upper_t * upper_t + 3.0 * upper_t * upper_t + 3.0 * upper_t + 1.0) / 6.0, upper_t * upper_t * upper_t / 6.0])
    slopes = jnp.stack([-0.5 * lower_t * lower_t, 0.5 * (3.0 * upper_t * upper_t - 4.0 * upper_t), 0.5 * (-3.0 * upper_t * upper_t + 2.0 * upper_t + 1.0), 0.5 * upper_t * upper_t])
    return (weights, slopes)

def frequency(waves):
    signed = jnp.where(waves <= MESH // 2, waves, waves - MESH).astype(jnp.float32) / MESH
    modulus = 9.0 / jnp.square(2.0 + jnp.cos(waves.astype(jnp.float32) * (2.0 * math.pi / MESH)))
    return (signed, modulus)

def influence(wave_y, wave_z, wave_x):
    freq_y, modul_y = frequency(wave_y)
    freq_z, modul_z = frequency(wave_z)
    freq_x, modul_x = frequency(wave_x)
    wave_square = jnp.square(freq_x)[None, None, :] + jnp.square(freq_y)[:, None, None] + jnp.square(freq_z)[None, :, None]
    positive = wave_square > 0.0
    gaussian = jnp.exp(-(math.pi * math.pi / (EWALD * EWALD)) * wave_square)
    kernel = jnp.where(positive, gaussian / jnp.where(positive, wave_square, 1.0), 0.0)
    moduli = modul_x[None, None, :] * modul_y[:, None, None] * modul_z[None, :, None]
    return kernel * moduli * (COULOMB / (math.pi * MESH ** 3))

def interact(current, lookup, places, located, links, radial_in, radial_out, mix_weight):
    atom_count = current.shape[0]
    gathered = lookup[links].astype(jnp.float32)
    displace = places[links] - located[None]
    length_sq = lax.optimization_barrier(jnp.sum(displace * displace, axis=-1))
    distance = jnp.sqrt(length_sq)
    direction = displace / jnp.sqrt(length_sq + 1.0)[..., None]
    spacing = ENV / (NB - 1)
    centres = jnp.arange(NB, dtype=jnp.float32) * spacing
    envelope = jnp.square(jnp.maximum(1.0 - length_sq / (ENV * ENV), 0.0))
    basis_set = jnp.exp(-jnp.square((distance[..., None] - centres) / spacing)) * envelope[..., None]
    edge_count = NEIGH * atom_count
    hidden = jax.nn.silu(jnp.dot(basis_set.reshape(edge_count, NB).astype(jnp.bfloat16), radial_in, preferred_element_type=jnp.float32)).astype(jnp.bfloat16)
    radial = jnp.dot(hidden, radial_out, preferred_element_type=jnp.float32).reshape(NEIGH, atom_count, 4 * C)
    scalars = gathered[..., :C]
    vectors = gathered[..., C:].reshape(NEIGH, atom_count, 3, C)
    first_path = radial[..., :C]
    second_path = radial[..., C:2 * C]
    third_path = radial[..., 2 * C:3 * C]
    fourth_path = radial[..., 3 * C:]
    projected = lax.optimization_barrier(jnp.sum(direction[..., None] * vectors, axis=2))
    inverse_root = 1.0 / math.sqrt(NEIGH)
    scalar_message = lax.optimization_barrier(jnp.sum(first_path * scalars + second_path * projected, axis=0)) * inverse_root
    scaled_path = third_path * scalars
    vector_message = (jnp.einsum('kad,kac->adc', direction, scaled_path, precision=lax.Precision.HIGHEST) + lax.optimization_barrier(jnp.sum(fourth_path[:, :, None, :] * vectors, axis=0))) * inverse_root
    previous = current.astype(jnp.float32)
    scalar_new = previous[:, :C] + jax.nn.silu(jnp.dot(scalar_message.astype(jnp.bfloat16), mix_weight[0], preferred_element_type=jnp.float32))
    vector_new = previous[:, C:] + jnp.dot(vector_message.reshape(atom_count * 3, C).astype(jnp.bfloat16), mix_weight[1], preferred_element_type=jnp.float32).reshape(atom_count, 3 * C)
    return jnp.concatenate([scalar_new, vector_new], axis=1).astype(jnp.bfloat16)

def ghost_values(values, octant_rows):
    width_last = values.shape[-1]
    flattened = octant_rows.reshape(N_GX, N_GY, N_GZ, 8 * GHOST, 1)
    flattened = jnp.broadcast_to(flattened, (N_GX, N_GY, N_GZ, 8 * GHOST, width_last))
    buffers = jnp.take_along_axis(values, flattened, axis=3).reshape(N_GX, N_GY, N_GZ, 8, GHOST, width_last)
    pieces = []
    for corner in outer_cells():
        roll_by = (-offset_of(corner[0]), -offset_of(corner[1]), -offset_of(corner[2]))
        octant = 4 * source_of(corner[0]) + 2 * source_of(corner[1]) + source_of(corner[2])
        pieces.append(jnp.roll(buffers[:, :, :, octant], roll_by, (0, 1, 2)))
    return jnp.concatenate(pieces, axis=3)

def reference(features, fraction, cell_index, species, octant_rows, neighbours, radial_in, radial_out, mix_weight, readout, species_table):
    device_total = N_GX * N_GY * N_GZ
    cell_float = jnp.swapaxes(cell_index, 3, 4).astype(jnp.float32)
    fraction_float = jnp.swapaxes(fraction, 3, 4).astype(jnp.float32)
    located = cell_float + fraction_float
    shift_list = []
    for corner in outer_cells():
        shift_list.append(jnp.array([offset_of(corner[0]) * BX, offset_of(corner[1]) * BY, offset_of(corner[2]) * BZ], jnp.float32))
    shift_rows = jnp.repeat(jnp.stack(shift_list), GHOST, axis=0)
    ghost_places = ghost_values(cell_float, octant_rows) + shift_rows + ghost_values(fraction_float, octant_rows)
    places = jnp.concatenate([located, ghost_places, jnp.zeros((N_GX, N_GY, N_GZ, 1, 3), jnp.float32)], axis=3)
    corners = outer_cells()
    offset_x = jnp.array([offset_of(corner[0]) for corner in corners], jnp.int32)
    offset_y = jnp.array([offset_of(corner[1]) for corner in corners], jnp.int32)
    offset_z = jnp.array([offset_of(corner[2]) for corner in corners], jnp.int32)
    octant_ids = jnp.array([4 * source_of(corner[0]) + 2 * source_of(corner[1]) + source_of(corner[2]) for corner in corners], jnp.int32)
    current_features = features
    for layer_index in range(LAYERS):

        def per_device(inputs, layer_index=layer_index, whole=current_features):
            device_id, current, places_one, located_one, links_one = inputs
            index_x = device_id // (N_GY * N_GZ)
            index_y = device_id // N_GZ % N_GY
            index_z = device_id % N_GZ
            source_x = (index_x + offset_x) % N_GX
            source_y = (index_y + offset_y) % N_GY
            source_z = (index_z + offset_z) % N_GZ
            rows = octant_rows[source_x, source_y, source_z, octant_ids]
            arrived = whole[source_x[:, None], source_y[:, None], source_z[:, None], rows].reshape(56 * GHOST, 4 * C)
            lookup_one = jnp.concatenate([current, arrived, jnp.zeros((1, 4 * C), jnp.bfloat16)], axis=0)
            return interact(current, lookup_one, places_one, located_one, links_one, radial_in[layer_index], radial_out[layer_index], mix_weight[layer_index])
        mapped = lax.map(per_device, (jnp.arange(device_total, dtype=jnp.int32), current_features.reshape(device_total, ATOMS, 4 * C), places.reshape(device_total, NCAND + 1, 3), located.reshape(device_total, ATOMS, 3), neighbours.reshape(device_total, NEIGH, ATOMS)))
        current_features = mapped.reshape(N_GX, N_GY, N_GZ, ATOMS, 4 * C)
    scalars = current_features[..., :C].reshape(-1, C)
    head_out = jnp.dot(scalars, readout, preferred_element_type=jnp.float32).reshape(N_GX, N_GY, N_GZ, ATOMS, 2)
    one_hot = (species[..., None] == jnp.arange(NSPEC, dtype=jnp.int32)).astype(jnp.float32).reshape(-1, NSPEC)
    species_term = jnp.dot(one_hot, species_table, precision=lax.Precision.HIGHEST, preferred_element_type=jnp.float32).reshape(N_GX, N_GY, N_GZ, ATOMS, 2)
    base_energy = head_out[..., 0] + species_term[..., 0]
    charge = head_out[..., 1] + species_term[..., 1]
    weights, slopes = spline(fraction.astype(jnp.float32))
    anchors = [(jnp.arange(N_GX, dtype=jnp.int32) * BX).reshape(N_GX, 1, 1, 1), (jnp.arange(N_GY, dtype=jnp.int32) * BY).reshape(1, N_GY, 1, 1), (jnp.arange(N_GZ, dtype=jnp.int32) * BZ).reshape(1, 1, N_GZ, 1)]
    offsets = jnp.arange(4, dtype=jnp.int32).reshape(4, 1, 1, 1, 1)
    points = [(anchors[dim][None] + cell_index[:, :, :, dim][None] + offsets - 1) % MESH for dim in range(3)]
    weight_x = weights[:, :, :, :, 0]
    weight_y = weights[:, :, :, :, 1]
    weight_z = weights[:, :, :, :, 2]
    slope_x = slopes[:, :, :, :, 0]
    slope_y = slopes[:, :, :, :, 1]
    slope_z = slopes[:, :, :, :, 2]
    point_x = points[0][:, None, None]
    point_y = points[1][None, :, None]
    point_z = points[2][None, None, :]
    amount = charge[None, None, None] * weight_x[:, None, None] * weight_y[None, :, None] * weight_z[None, None, :]
    charge_mesh = jnp.zeros((MESH, MESH, MESH), jnp.float32).at[point_x, point_y, point_z].add(amount)
    waves = jnp.arange(MESH, dtype=jnp.int32)
    kernel = jnp.transpose(influence(waves, waves, waves), (2, 0, 1))
    spectrum = jnp.fft.fftn(charge_mesh)
    potential = jnp.real(jnp.fft.ifftn(spectrum * kernel)) * float(MESH ** 3)
    sampled = potential[point_x, point_y, point_z]
    potential_at = lax.optimization_barrier(jnp.sum(sampled * weight_x[:, None, None] * weight_y[None, :, None] * weight_z[None, None, :], axis=(0, 1, 2)))
    field_x = -lax.optimization_barrier(jnp.sum(sampled * slope_x[:, None, None] * weight_y[None, :, None] * weight_z[None, None, :], axis=(0, 1, 2)))
    field_y = -lax.optimization_barrier(jnp.sum(sampled * weight_x[:, None, None] * slope_y[None, :, None] * weight_z[None, None, :], axis=(0, 1, 2)))
    field_z = -lax.optimization_barrier(jnp.sum(sampled * weight_x[:, None, None] * weight_y[None, :, None] * slope_z[None, None, :], axis=(0, 1, 2)))
    recip_force = charge[:, :, :, None] * jnp.stack([field_x, field_y, field_z], axis=3)
    site_energy = base_energy + 0.5 * charge * potential_at
    return (current_features, site_energy, recip_force)
```

```python
import math

import jax
import jax.numpy as jnp
import numpy as np
from jax import lax
from jax.experimental import pallas as pl
from jax.experimental.pallas import tpu as pltpu
from jax.sharding import PartitionSpec as P

C = 128
NB = 8
HID = 64
NEIGH = 16
ENV = 7
MESH = 256
ATOMS = 128
COULOMB = 4.0
EWALD = 0.7
BX, BY, BZ = 16, 128, 32
ZPAD = 40

F32 = jnp.float32
BF16 = jnp.bfloat16
NN = (((1,), (0,)), ((), ()))
NT = (((1,), (1,)), ((), ()))
TN = (((0,), (0,)), ((), ()))


def dot(a, b, dims=NN):
    return lax.dot_general(a, b, dims, preferred_element_type=F32)


def halves(x):
    high = x.astype(BF16)
    return high, (x - high.astype(F32)).astype(BF16)


def dot3(a, b, dims=NN):
    return dot(a[0], b[0], dims) + (dot(a[0], b[1], dims) + dot(a[1], b[0], dims))


def np_halves(x):
    x = np.asarray(x, np.float32)
    high = x.astype(BF16)
    return high, (x - high.astype(np.float32)).astype(BF16)


def real_basis():
    rows = np.arange(MESH)
    wave = np.where(rows <= MESH // 2, rows, rows - MESH // 2)
    angle = 2.0 * np.pi * ((wave[:, None] * np.arange(MESH)[None, :]) % MESH) / MESH
    table = np.where((rows <= MESH // 2)[:, None], np.cos(angle), np.sin(angle))
    return wave, table


def constants():
    wave, table = real_basis()
    freq = wave / MESH
    modulus = 9.0 / np.square(2.0 + np.cos(2.0 * np.pi * wave / MESH))
    weight = np.where((wave == 0) | (wave == MESH // 2), 1.0, 2.0)
    factor = np.exp(-(np.pi**2 / EWALD**2) * freq**2) * modulus * weight
    out = {"basis_y": np_halves(table)}
    zed = np.zeros((8, 128, MESH))
    for part in range(8):
        for point in range(35):
            zed[part, point] = table[:, (part * BZ + point - 1) % MESH]
    out["basis_z"] = np_halves(zed.reshape(1024, MESH))
    exx = np.zeros((3, MESH, 16, 8))
    for third in range(3):
        for part in range(16):
            for group in range(7):
                point = 3 * group + third
                if point < 19:
                    exx[third, :, part, group] = table[:, (part * BX + point - 1) % MESH]
    exx = exx.reshape(3, MESH, 128)
    out["basis_x"] = np_halves(exx)
    out["basis_xt"] = np_halves(np.swapaxes(exx, 1, 2))
    out["col"] = np.stack([freq**2, factor], axis=1).astype(np.float32)
    row = np.zeros((8, MESH), np.float32)
    row[0], row[1] = freq**2, factor
    out["row"] = row
    out["scale_y"] = (factor * (COULOMB / (math.pi * MESH**3))).astype(np.float32)
    return out


def select_rows(octants):
    wanted = jnp.transpose(jnp.broadcast_to(octants.astype(F32), (128, 128)))
    lane = lax.broadcasted_iota(jnp.int32, (128, 128), 1).astype(F32)
    return jnp.where(wanted == lane, 1.0, 0.0).astype(BF16)


def geometry_rows(cells, fraction):
    return jnp.concatenate(
        [cells.astype(F32), fraction.astype(F32), jnp.zeros((122, ATOMS), F32)], axis=0
    )


def prep_kernel(feats, fraction, cells, octants, out):
    chosen = select_rows(octants[...])
    out[:, :512] = dot(chosen, feats[...]).astype(BF16)
    geometry = jnp.transpose(geometry_rows(cells[...], fraction[...])).astype(BF16)
    out[:, 512:] = dot(chosen, geometry).astype(BF16)


def table_rows(neighbours):
    ghost = neighbours - ATOMS
    outer = (ghost * 4682) >> 16
    spot = ghost - outer * 14
    code = outer
    for bound in (21, 21, 23, 23, 33, 33, 35, 35):
        code = code + (outer >= bound).astype(jnp.int32)
    ex, ey, ez = code >> 4, (code >> 2) & 3, code & 3
    is_ghost = (neighbours >= ATOMS) & (neighbours < 912)
    near = (ey == 1) | (ey == 2)
    half = jnp.where(near, ey - 1, jnp.where(ey == 0, 1, 0))
    base = jnp.where(near, 128, 640)
    row = base + ((ex * 2 + half) * 4 + ez) * 16 + spot
    row = jnp.where(is_ghost, row, jnp.where(neighbours < ATOMS, neighbours, -1))

    def offset(coord, span):
        moved = jnp.where(coord == 3, span, jnp.where(coord == 0, -span, 0))
        return jnp.where(is_ghost, moved, 0).astype(F32)

    return row, (offset(ex, BX), offset(ey, BY), offset(ez, BZ))


def transposed(x):
    return jnp.transpose(x.astype(F32)).astype(BF16)


def gather_slots(rows, table, gathered, geometry=None):
    for pair in range(NEIGH // 2):
        wanted = jnp.concatenate(
            [rows[2 * pair : 2 * pair + 1, :], rows[2 * pair + 1 : 2 * pair + 2, :]], axis=1
        )
        spots = lax.broadcasted_iota(jnp.int32, (1152, 256), 0)
        one_hot = jnp.where(spots == wanted, 1.0, 0.0).astype(BF16)
        found = dot(table[...], one_hot)
        lanes = slice(pair * 256, pair * 256 + 256)
        gathered[:, lanes] = found[:512].astype(BF16)
        if geometry is not None:
            geometry[:, lanes] = found[512:520]


def silu(x):
    return x * (1.0 / (1.0 + jnp.exp(-x)))


def messages(hidden, radial_out, radial, gathered, unit, message):
    for pair in range(NEIGH // 2):
        lanes = slice(pair * 256, pair * 256 + 256)
        radial[:, lanes] = dot(radial_out, hidden[:, lanes], TN)

    def one_chunk(chunk, carry):
        start = pl.multiple_of(chunk * 32, 32)
        sums = [jnp.zeros((32, 128), F32) for _ in range(4)]
        for slot in range(NEIGH):
            lanes = slice(slot * 128, slot * 128 + 128)
            r = [radial[pl.ds(start + 128 * p, 32), lanes] for p in range(4)]
            s, vx, vy, vz = [
                gathered[pl.ds(start + 128 * p, 32), lanes].astype(F32) for p in range(4)
            ]
            ux = unit[slot : slot + 1, :]
            uy = unit[16 + slot : 17 + slot, :]
            uz = unit[32 + slot : 33 + slot, :]
            sums[0] += r[0] * s + r[1] * (ux * vx + uy * vy + uz * vz)
            scaled = r[2] * s
            sums[1] += ux * scaled + r[3] * vx
            sums[2] += uy * scaled + r[3] * vy
            sums[3] += uz * scaled + r[3] * vz
        for p in range(4):
            message[pl.ds(start + 128 * p, 32), :] = (sums[p] * 0.25).astype(BF16)
        return carry

    lax.fori_loop(0, 4, one_chunk, 0)


def mixed(feats, message, mix_weight, layer, out):
    previous = feats[...].astype(F32)
    scalar = dot(message[0:128, :], mix_weight[layer, 0], TN)
    out[:, 0:128] = (previous[:, 0:128] + silu(scalar)).astype(BF16)
    for d in range(1, 4):
        rows = slice(128 * d, 128 * d + 128)
        moved = dot(message[rows, :], mix_weight[layer, 1], TN)
        out[:, rows] = (previous[:, rows] + moved).astype(BF16)


def first_kernel(
    feats, near, far, fraction, cells, octants, neighbours, radial_in, radial_out, mix_weight,
    new, outgoing, unit, hidden_next, rows_out,
    table, gathered, geometry, radial, message,
):
    table[:512, 0:128] = transposed(feats[...])
    table[512:528, 0:128] = geometry_rows(cells[...], fraction[...])[:16].astype(BF16)
    for start, piece in ((128, near), (640, far)):
        for q in range(4):
            lanes = slice(start + 128 * q, start + 128 * q + 128)
            flipped = transposed(piece[128 * q : 128 * q + 128, :])
            table[:, lanes] = flipped[:528]
    rows, shifts = table_rows(neighbours[...])
    rows_out[...] = rows
    gather_slots(rows, table, gathered, geometry)
    located = cells[...].astype(F32) + fraction[...].astype(F32)
    delta = []
    for d in range(3):
        cell = jnp.concatenate(
            [geometry[d : d + 1, k * 128 : k * 128 + 128] for k in range(NEIGH)], axis=0
        )
        part = jnp.concatenate(
            [geometry[3 + d : 4 + d, k * 128 : k * 128 + 128] for k in range(NEIGH)], axis=0
        )
        delta.append(((cell + shifts[d]) + part) - located[d : d + 1, :])
    length_sq = delta[0] * delta[0] + delta[1] * delta[1] + delta[2] * delta[2]
    distance = jnp.sqrt(length_sq)
    divisor = jnp.sqrt(length_sq + 1.0)
    for d in range(3):
        unit[16 * d : 16 * d + 16, :] = delta[d] / divisor
    envelope = jnp.square(jnp.maximum(1.0 - length_sq / (ENV * ENV), 0.0))
    centres = lax.broadcasted_iota(jnp.int32, (NB, 128), 0).astype(F32)
    basis = []
    for k in range(NEIGH):
        away = distance[k : k + 1, :] - centres
        basis.append(jnp.exp(-(away * away)) * envelope[k : k + 1, :])
    basis = jnp.concatenate(basis, axis=1).astype(BF16)
    hidden = silu(dot(radial_in[0], basis, TN)).astype(BF16)
    hidden_next[...] = silu(dot(radial_in[1], basis, TN)).astype(BF16)
    messages(hidden, radial_out[0], radial, gathered, unit, message)
    mixed(feats, message, mix_weight, 0, new)
    outgoing[...] = dot(select_rows(octants[...]), new[...]).astype(BF16)


def second_kernel(
    feats, near, far, rows, unit, hidden, radial_out, mix_weight, readout, kinds, species_table,
    fraction, cells,
    new, packed, base,
    table, gathered, radial, message,
):
    table[:, 0:128] = transposed(feats[...])
    for start, piece in ((128, near), (640, far)):
        for q in range(4):
            lanes = slice(start + 128 * q, start + 128 * q + 128)
            table[:, lanes] = transposed(piece[128 * q : 128 * q + 128, :])
    gather_slots(rows[...], table, gathered)
    messages(hidden[...], radial_out[1], radial, gathered, unit, message)
    mixed(feats, message, mix_weight, 1, new)
    heads = dot(readout[...], new[:, 0:128], NT)
    second = kinds[...] == 1
    energy = jnp.where(second, species_table[1, 0], species_table[0, 0])
    offset = jnp.where(second, species_table[1, 1], species_table[0, 1])
    base[...] = heads[0:1, :] + energy
    packed[...] = jnp.concatenate(
        [
            heads[1:2, :] + offset,
            fraction[...].astype(F32),
            cells[...].astype(F32),
            jnp.zeros((1, ATOMS), F32),
        ],
        axis=0,
    )


def spline(t):
    s = 1.0 - t
    weights = [
        s * s * s / 6.0,
        (3.0 * t * t * t - 6.0 * t * t + 4.0) / 6.0,
        (-3.0 * t * t * t + 3.0 * t * t + 3.0 * t + 1.0) / 6.0,
        t * t * t / 6.0,
    ]
    slopes = [
        -0.5 * s * s,
        0.5 * (3.0 * t * t - 4.0 * t),
        0.5 * (-3.0 * t * t + 2.0 * t + 1.0),
        0.5 * t * t,
    ]
    return weights, slopes


def spread(coefficients, spots, count):
    row = lax.broadcasted_iota(jnp.int32, (count, spots[0].shape[1]), 0)
    total = jnp.zeros(row.shape, F32)
    for coefficient, spot in zip(coefficients, spots):
        total = jnp.where(row == spot, coefficient, total)
    return total


def planes_of(along_x, along_z):
    tail = jnp.zeros((8, along_z.shape[1]), F32)
    tiles = []
    for group in range(7):
        parts = [along_z * along_x[3 * group + c : 3 * group + c + 1, :] for c in range(3)]
        tiles.append(jnp.concatenate(parts + [tail], axis=0))
    return tiles


def both_atoms(own, other):
    both = jnp.concatenate([own[...], other[...]], axis=1)
    return both, [both[4 + d : 5 + d, :].astype(jnp.int32) for d in range(3)]


def charges_kernel(own, other, high, low, out, weight_y, slope_y):
    both, cells = both_atoms(own, other)
    half = lax.axis_index("gy")
    lane = lax.broadcasted_iota(jnp.int32, (1, 256), 1)
    domain = jnp.where(lane < 128, half, 1 - half)
    rows = pl.ds(pl.multiple_of(half * 128, 128), 128)
    table = (high[rows, :], low[rows, :])
    weights, slopes = spline(both[2:3, :])
    spots = [(cells[1] + domain * BY + (m - 1)) & (MESH - 1) for m in range(4)]
    along_y = dot3(table, halves(spread(weights, spots, MESH)))
    weight_y[...] = along_y
    slope_y[...] = dot3(table, halves(spread(slopes, spots, MESH)))
    charged = halves(along_y * both[0:1, :])
    along_x = spread(spline(both[1:2, :])[0], [cells[0] + m for m in range(4)], 24)
    along_z = spread(spline(both[3:4, :])[0], [cells[2] + m for m in range(4)], ZPAD)
    for group, tile in enumerate(planes_of(along_x, along_z)):
        out[:, group, :] = dot3(charged, halves(tile), NT)
    out[:, 7, :] = jnp.zeros((128, 128), F32)


def waves_kernel(
    scale_y, received, zh, zl, xh, xl, th, tl, col, row, out, lhs,
):
    for part in range(8):
        lanes = slice(part * 128, part * 128 + 128)
        block = received[part]
        for third in range(3):
            moved = block if third == 0 else pltpu.roll(block, 128 - ZPAD * third, 1)
            lhs[third * 128 : third * 128 + 128, lanes] = moved
    zed = (zh[...], zl[...])
    lines = dot3(halves(lhs[...]), zed)
    total = jnp.zeros((MESH, MESH), F32)
    for third in range(3):
        total += dot3(
            (xh[third], xl[third]), halves(lines[third * 128 : third * 128 + 128, :])
        )
    number = lax.axis_index("gy") * 128 + lax.axis_index("gz") * 16 + lax.axis_index("gx")
    wave = jnp.where(number <= 128, number, number - 128)
    freq_y = wave.astype(F32) / MESH
    square = (col[:, 0:1] + row[0:1, :]) + freq_y * freq_y
    kernel = (col[:, 1:2] * scale_y[number]) * row[1:2, :]
    positive = square > 0.0
    kernel = jnp.where(positive, kernel / jnp.where(positive, square, 1.0), 0.0)
    scaled = halves(total * kernel)
    for third in range(3):
        lhs[third * 128 : third * 128 + 128, :] = dot3(
            halves(dot3((th[third], tl[third]), scaled)), zed, NT
        )
    for part in range(8):
        lanes = slice(part * 128, part * 128 + 128)
        block = lhs[0:128, lanes]
        for third in range(1, 3):
            block += pltpu.roll(lhs[third * 128 : third * 128 + 128, lanes], ZPAD * third, 1)
        out[part] = block


def forces_kernel(own, other, weight_y, slope_y, returned, out_own, out_other):
    both, cells = both_atoms(own, other)
    flat = halves(jnp.concatenate([returned[:, group, :] for group in range(7)], axis=1))
    weights_x, slopes_x = spline(both[1:2, :])
    weights_z, slopes_z = spline(both[3:4, :])
    spots_x = [cells[0] + m for m in range(4)]
    spots_z = [cells[2] + m for m in range(4)]
    along_x = spread(weights_x, spots_x, 24)
    along_z = spread(weights_z, spots_z, ZPAD)
    down_x = spread(slopes_x, spots_x, 24)
    down_z = spread(slopes_z, spots_z, ZPAD)

    def level(ax, az):
        return dot3(flat, halves(jnp.concatenate(planes_of(ax, az), axis=0)))

    level_0 = level(along_x, along_z)
    wy = weight_y[...]
    rows = [
        jnp.sum(wy * level_0, axis=0, keepdims=True),
        jnp.sum(wy * level(down_x, along_z), axis=0, keepdims=True),
        jnp.sum(slope_y[...] * level_0, axis=0, keepdims=True),
        jnp.sum(wy * level(along_x, down_z), axis=0, keepdims=True),
        jnp.zeros((4, 256), F32),
    ]
    total = jnp.concatenate(rows, axis=0)
    out_own[...] = total[:, 0:128]
    out_other[...] = total[:, 128:256]


VMEM = pl.BlockSpec(memory_space=pltpu.VMEM)
SMEM = pl.BlockSpec(memory_space=pltpu.SMEM)


def call(kernel, outs, *args, scratch=(), scalars=()):
    specs = [SMEM if i in scalars else VMEM for i in range(len(args))]
    return pl.pallas_call(
        kernel,
        out_shape=[jax.ShapeDtypeStruct(s, d) for s, d in outs],
        in_specs=specs,
        out_specs=[VMEM] * len(outs),
        scratch_shapes=[pltpu.VMEM(s, d) for s, d in scratch],
    )(*args)


def ring(axis, step):
    count = lax.axis_size(axis)
    return [(i, (i + step) % count) for i in range(count)]


def partner(block):
    return lax.ppermute(block, "gy", [(0, 1), (1, 0)])


def ghosts(blocks):
    width = blocks.shape[1]
    x = blocks.reshape(2, 2, 2, 16, width)
    before = lax.ppermute(x[:, :, 1:], "gz", ring("gz", 1))
    after = lax.ppermute(x[:, :, :1], "gz", ring("gz", -1))
    x = jnp.concatenate([before, x, after], axis=2)
    before = lax.ppermute(x[1:], "gx", ring("gx", 1))
    after = lax.ppermute(x[:1], "gx", ring("gx", -1))
    x = jnp.concatenate([before, x, after], axis=0)
    return x.reshape(512, width), partner(x).reshape(512, width)


def across(blocks):
    return lax.all_to_all(blocks, ("gz", "gx"), split_axis=0, concat_axis=0, tiled=True)


def per_device(
    features, fraction, cell_index, species, octant_rows, neighbours,
    radial_in, radial_out, mix_weight, readout, species_table,
):
    table = constants()
    feats = features[0, 0, 0]
    part = fraction[0, 0, 0]
    cells = cell_index[0, 0, 0]
    kinds = species.reshape(1, ATOMS)
    octants = jnp.pad(octant_rows[0, 0, 0], ((0, 0), (0, 2)), constant_values=-1).reshape(1, 128)
    links = neighbours[0, 0, 0]
    heads = jnp.pad(jnp.transpose(readout), ((0, 6), (0, 0)))

    (outgoing,) = call(prep_kernel, [((128, 640), BF16)], feats, part, cells, octants)
    near, far = ghosts(outgoing)
    feats, outgoing, unit, hidden, rows = call(
        first_kernel,
        [
            ((128, 512), BF16),
            ((128, 512), BF16),
            ((48, 128), F32),
            ((HID, 2048), BF16),
            ((NEIGH, 128), jnp.int32),
        ],
        feats, near, far, part, cells, octants, links, radial_in, radial_out, mix_weight,
        scratch=[
            ((528, 1152), BF16),
            ((512, 2048), BF16),
            ((8, 2048), F32),
            ((512, 2048), F32),
            ((512, 128), BF16),
        ],
    )
    near, far = ghosts(outgoing)
    feats, packed, base = call(
        second_kernel,
        [((128, 512), BF16), ((8, 128), F32), ((1, 128), F32)],
        feats, near, far, rows, unit, hidden, radial_out, mix_weight, heads, kinds, species_table,
        part, cells,
        scalars=(10,),
        scratch=[
            ((512, 1152), BF16),
            ((512, 2048), BF16),
            ((512, 2048), F32),
            ((512, 128), BF16),
        ],
    )
    other = partner(packed)
    lines, weight_y, slope_y = call(
        charges_kernel,
        [((128, 8, 128), F32), ((128, 256), F32), ((128, 256), F32)],
        packed, other, *table["basis_y"],
    )
    received = across(lines).reshape(8, 128, 128)
    (waves,) = call(
        waves_kernel,
        [((8, 128, 128), F32)],
        table["scale_y"], received, *table["basis_z"], *table["basis_x"], *table["basis_xt"],
        table["col"], table["row"],
        scalars=(0,),
        scratch=[((384, 1024), F32)],
    )
    returned = across(waves.reshape(128, 8, 128))
    here, there = call(
        forces_kernel,
        [((8, 128), F32), ((8, 128), F32)],
        packed, other, weight_y, slope_y, returned,
    )
    total = here + partner(there)
    charge = packed[0:1]
    force = -charge * total[1:4]
    energy = base + 0.5 * charge * total[0:1]
    return feats[None, None, None], energy.reshape(1, 1, 1, ATOMS), force[None, None, None]


def solution(mesh):
    domain = P("gx", "gy", "gz", None, None)
    atoms = P("gx", "gy", "gz", None)
    return jax.shard_map(
        per_device,
        mesh=mesh,
        in_specs=(domain, domain, domain, atoms, domain, domain, P(), P(), P(), P(), P()),
        out_specs=(domain, atoms, domain),
        check_vma=False,
    )
```

```python
import math

import jax
import jax.numpy as jnp
import numpy as np
from jax import lax
from jax.experimental import pallas as pl
from jax.experimental.pallas import tpu as pltpu
from jax.sharding import PartitionSpec as P

C = 128
NB = 8
HID = 64
NEIGH = 16
ENV = 7
MESH = 256
ATOMS = 128
COULOMB = 4.0
EWALD = 0.7
BX, BY, BZ = 16, 128, 32
ZPAD = 40

NODES = (1, 9, 17, 25, 33)

F32 = jnp.float32
BF16 = jnp.bfloat16
NN = (((1,), (0,)), ((), ()))
NT = (((1,), (1,)), ((), ()))
TN = (((0,), (0,)), ((), ()))


def dot(a, b, dims=NN):
    return lax.dot_general(a, b, dims, preferred_element_type=F32)


def halves(x):
    high = x.astype(BF16)
    return high, (x - high.astype(F32)).astype(BF16)


def dot3(a, b, dims=NN):
    return dot(a[0], b[0], dims) + (dot(a[0], b[1], dims) + dot(a[1], b[0], dims))


def np_halves(x):
    x = np.asarray(x, np.float32)
    high = x.astype(BF16)
    return high, (x - high.astype(np.float32)).astype(BF16)


def real_basis():
    rows = np.arange(MESH)
    wave = np.where(rows <= MESH // 2, rows, rows - MESH // 2)
    angle = 2.0 * np.pi * ((wave[:, None] * np.arange(MESH)[None, :]) % MESH) / MESH
    table = np.where((rows <= MESH // 2)[:, None], np.cos(angle), np.sin(angle))
    return wave, table


def constants():
    wave, table = real_basis()
    freq = wave / MESH
    modulus = 9.0 / np.square(2.0 + np.cos(2.0 * np.pi * wave / MESH))
    weight = np.where((wave == 0) | (wave == MESH // 2), 1.0, 2.0)
    factor = np.exp(-(np.pi**2 / EWALD**2) * freq**2) * modulus * weight
    out = {"basis_y": np_halves(table)}
    zed = np.zeros((8, 128, MESH))
    for part in range(8):
        for point in range(35):
            zed[part, point] = table[:, (part * BZ + point - 1) % MESH]
        for spare, node in enumerate(NODES):
            zed[part, 35 + spare] = table[:, (part * BZ + node - 1) % MESH]
    carry = np.zeros((128, 128), np.float32)
    for point in range(35):
        left = min(max((point - 1) // 8, 0), 3)
        share = (point - NODES[left]) / 8.0
        for third in range(3):
            row = ZPAD * third + point
            carry[row, ZPAD * third + 35 + left] = 1.0 - share
            carry[row, ZPAD * third + 36 + left] = share
    out["carry"] = carry.astype(BF16)
    out["basis_z"] = np_halves(zed.reshape(1024, MESH))
    exx = np.zeros((3, MESH, 16, 8))
    for third in range(3):
        for part in range(16):
            for group in range(7):
                point = 3 * group + third
                if point < 19:
                    exx[third, :, part, group] = table[:, (part * BX + point - 1) % MESH]
    exx = exx.reshape(3, MESH, 128)
    out["basis_x"] = np_halves(exx)
    out["basis_xt"] = np_halves(np.swapaxes(exx, 1, 2))
    out["col"] = np.stack([freq**2, factor], axis=1).astype(np.float32)
    row = np.zeros((8, MESH), np.float32)
    row[0], row[1] = freq**2, factor
    out["row"] = row
    out["scale_y"] = (factor * (COULOMB / (math.pi * MESH**3))).astype(np.float32)
    return out


def select_rows(octants):
    slot = lax.broadcasted_iota(jnp.int32, (128, 8), 0)
    group = lax.broadcasted_iota(jnp.int32, (128, 8), 1)
    picker = jnp.where((slot >> 4) == group, 1.0, 0.0).astype(BF16)
    listed = dot(picker, octants[...].astype(F32).astype(BF16))
    spot = lax.broadcasted_iota(jnp.int32, listed.shape, 0) & 15
    entry = lax.broadcasted_iota(jnp.int32, listed.shape, 1)
    wanted = jnp.sum(jnp.where(spot == entry, listed, 0.0), axis=1, keepdims=True)
    lane = lax.broadcasted_iota(jnp.int32, (128, 128), 1).astype(F32)
    return jnp.where(wanted == lane, 1.0, 0.0).astype(BF16)


def cell_rows(cells):
    return [cells[:, 128 * d : 128 * d + 128].astype(F32) for d in range(3)]


def geometry_rows(cells, fraction):
    return jnp.concatenate(
        cell_rows(cells) + [fraction[...].astype(F32), jnp.zeros((122, ATOMS), F32)], axis=0
    )


def prep_kernel(feats, fraction, cells, octants, out, geometry_out):
    chosen = select_rows(octants)
    out[:, :512] = dot(chosen, feats[...]).astype(BF16)
    geometry = geometry_rows(cells, fraction)
    out[:, 512:] = dot(chosen, jnp.transpose(geometry).astype(BF16)).astype(BF16)
    geometry_out[...] = geometry[0:8]


def table_rows(neighbours):
    ghost = neighbours - ATOMS
    outer = (ghost * 4682) >> 16
    spot = ghost - outer * 14
    code = outer
    for bound in (21, 21, 23, 23, 33, 33, 35, 35):
        code = code + (outer >= bound).astype(jnp.int32)
    ex, ey, ez = code >> 4, (code >> 2) & 3, code & 3
    is_ghost = (neighbours >= ATOMS) & (neighbours < 912)
    near = (ey == 1) | (ey == 2)
    half = jnp.where(near, ey - 1, jnp.where(ey == 0, 1, 0))
    base = jnp.where(near, 0, 512)
    row = base + ((ex * 2 + half) * 4 + ez) * 16 + spot
    own = 144 + ((neighbours >> 5) << 6) + (neighbours & 31)
    row = jnp.where(is_ghost, row, jnp.where(neighbours < ATOMS, own, -1))

    def offset(coord, span):
        moved = jnp.where(coord == 3, span, jnp.where(coord == 0, -span, 0))
        return jnp.where(is_ghost, moved, 0).astype(F32)

    return row, (offset(ex, BX), offset(ey, BY), offset(ez, BZ))


def transposed(x):
    return jnp.transpose(x.astype(F32)).astype(BF16)


def fill_table(table, feats, near, far, count, geometry=None):
    own = feats[...]
    if geometry is not None:
        own = jnp.concatenate([own, geometry], axis=1)
    for q in range(4):
        piece = near[128 * q : 128 * q + 128, :]
        if q in (1, 2):
            at = 64 * (q - 1)
            piece = jnp.concatenate(
                [
                    piece[0:16], own[at : at + 32], piece[48:80], own[at + 32 : at + 64],
                    piece[112:128],
                ],
                axis=0,
            )
        table[:, 128 * q : 128 * q + 128] = transposed(piece)[:count]
        piece = far[128 * q : 128 * q + 128, :]
        table[:, 512 + 128 * q : 640 + 128 * q] = transposed(piece)[:count]


def gather_slots(rows, table, gathered, geometry=None):
    for pair in range(NEIGH // 2):
        wanted = jnp.concatenate(
            [rows[2 * pair : 2 * pair + 1, :], rows[2 * pair + 1 : 2 * pair + 2, :]], axis=1
        )
        spots = lax.broadcasted_iota(jnp.int32, (1024, 256), 0)
        one_hot = jnp.where(spots == wanted, 1.0, 0.0).astype(BF16)
        found = dot(table[...], one_hot)
        lanes = slice(pair * 256, pair * 256 + 256)
        gathered[:, lanes] = found[:512].astype(BF16)
        if geometry is not None:
            geometry[:, lanes] = found[512:520]


def silu(x):
    return x * (1.0 / (1.0 + jnp.exp(-x)))


def messages(hidden, radial_out, radial, gathered, unit, message):
    for pair in range(NEIGH // 2):
        lanes = slice(pair * 256, pair * 256 + 256)
        radial[:, lanes] = dot(radial_out, hidden[:, lanes], TN)

    def one_chunk(chunk, carry):
        start = pl.multiple_of(chunk * 32, 32)
        sums = [jnp.zeros((32, 128), F32) for _ in range(4)]
        for slot in range(NEIGH):
            lanes = slice(slot * 128, slot * 128 + 128)
            r = [radial[pl.ds(start + 128 * p, 32), lanes] for p in range(4)]
            s, vx, vy, vz = [
                gathered[pl.ds(start + 128 * p, 32), lanes].astype(F32) for p in range(4)
            ]
            ux = unit[slot : slot + 1, :]
            uy = unit[16 + slot : 17 + slot, :]
            uz = unit[32 + slot : 33 + slot, :]
            sums[0] += r[0] * s + r[1] * (ux * vx + uy * vy + uz * vz)
            scaled = r[2] * s
            sums[1] += ux * scaled + r[3] * vx
            sums[2] += uy * scaled + r[3] * vy
            sums[3] += uz * scaled + r[3] * vz
        for p in range(4):
            message[pl.ds(start + 128 * p, 32), :] = (sums[p] * 0.25).astype(BF16)
        return carry

    lax.fori_loop(0, 4, one_chunk, 0)


def mixed(feats, message, mix_weight, layer, out):
    previous = feats[...].astype(F32)
    scalar = dot(message[0:128, :], mix_weight[layer, 0], TN)
    out[:, 0:128] = (previous[:, 0:128] + silu(scalar)).astype(BF16)
    for d in range(1, 4):
        rows = slice(128 * d, 128 * d + 128)
        moved = dot(message[rows, :], mix_weight[layer, 1], TN)
        out[:, rows] = (previous[:, rows] + moved).astype(BF16)


def first_kernel(
    feats, near, far, fraction, cells, octants, neighbours, radial_in, radial_out, mix_weight,
    new, outgoing, unit, hidden_next, rows_out,
    table, gathered, geometry, radial, message,
):
    own = jnp.transpose(geometry_rows(cells, fraction)).astype(BF16)
    fill_table(table, feats, near, far, 528, own)
    rows, shifts = table_rows(neighbours[...])
    rows_out[...] = rows
    gather_slots(rows, table, gathered, geometry)
    located = jnp.concatenate(cell_rows(cells), axis=0) + fraction[...].astype(F32)
    delta = []
    for d in range(3):
        cell = jnp.concatenate(
            [geometry[d : d + 1, k * 128 : k * 128 + 128] for k in range(NEIGH)], axis=0
        )
        part = jnp.concatenate(
            [geometry[3 + d : 4 + d, k * 128 : k * 128 + 128] for k in range(NEIGH)], axis=0
        )
        delta.append(((cell + shifts[d]) + part) - located[d : d + 1, :])
    length_sq = delta[0] * delta[0] + delta[1] * delta[1] + delta[2] * delta[2]
    distance = jnp.sqrt(length_sq)
    divisor = jnp.sqrt(length_sq + 1.0)
    for d in range(3):
        unit[16 * d : 16 * d + 16, :] = delta[d] / divisor
    envelope = jnp.square(jnp.maximum(1.0 - length_sq / (ENV * ENV), 0.0))
    centres = lax.broadcasted_iota(jnp.int32, (NB, 128), 0).astype(F32)
    basis = []
    for k in range(NEIGH):
        away = distance[k : k + 1, :] - centres
        basis.append(jnp.exp(-(away * away)) * envelope[k : k + 1, :])
    basis = jnp.concatenate(basis, axis=1).astype(BF16)
    hidden = silu(dot(radial_in[0], basis, TN)).astype(BF16)
    hidden_next[...] = silu(dot(radial_in[1], basis, TN)).astype(BF16)
    messages(hidden, radial_out[0], radial, gathered, unit, message)
    mixed(feats, message, mix_weight, 0, new)
    outgoing[...] = dot(select_rows(octants), new[...]).astype(BF16)


def second_kernel(
    feats, near, far, rows, unit, hidden, radial_out, mix_weight, readout, kinds, species_table,
    new, charge, base,
    table, gathered, radial, message,
):
    fill_table(table, feats, near, far, 512)
    gather_slots(rows[...], table, gathered)
    messages(hidden[...], radial_out[1], radial, gathered, unit, message)
    mixed(feats, message, mix_weight, 1, new)
    heads = dot(readout[...], new[:, 0:128], NT)
    second = kinds[...] == 1
    energy = jnp.where(second, species_table[1, 0], species_table[0, 0])
    offset = jnp.where(second, species_table[1, 1], species_table[0, 1])
    base[...] = heads[0:1, :] + energy
    charge[...] = heads[1:2, :] + offset


def spline(t):
    s = 1.0 - t
    weights = [
        s * s * s / 6.0,
        (3.0 * t * t * t - 6.0 * t * t + 4.0) / 6.0,
        (-3.0 * t * t * t + 3.0 * t * t + 3.0 * t + 1.0) / 6.0,
        t * t * t / 6.0,
    ]
    slopes = [
        -0.5 * s * s,
        0.5 * (3.0 * t * t - 4.0 * t),
        0.5 * (-3.0 * t * t + 2.0 * t + 1.0),
        0.5 * t * t,
    ]
    return weights, slopes


def spread(coefficients, spots, count):
    row = lax.broadcasted_iota(jnp.int32, (count, spots[0].shape[1]), 0)
    total = jnp.zeros(row.shape, F32)
    for coefficient, spot in zip(coefficients, spots):
        total = jnp.where(row == spot, coefficient, total)
    return total


def planes_of(along_x, along_z):
    tail = jnp.zeros((8, along_z.shape[1]), F32)
    tiles = []
    for group in range(7):
        parts = [along_z * along_x[3 * group + c : 3 * group + c + 1, :] for c in range(3)]
        tiles.append(jnp.concatenate(parts + [tail], axis=0))
    return tiles


def static_kernel(own, other, high, low, weight_y, slope_y, planes):
    both = jnp.concatenate([own[...], other[...]], axis=1)
    cells = [both[d : d + 1, :].astype(jnp.int32) for d in range(3)]
    half = lax.axis_index("gy")
    lane = lax.broadcasted_iota(jnp.int32, (1, 256), 1)
    domain = jnp.where(lane < 128, half, 1 - half)
    rows = pl.ds(pl.multiple_of(half * 128, 128), 128)
    table = (high[rows, :], low[rows, :])
    weights, slopes = spline(both[4:5, :])
    spots = [(cells[1] + domain * BY + (m - 1)) & (MESH - 1) for m in range(4)]
    weight_y[...] = dot3(table, halves(spread(weights, spots, MESH)))
    slope_y[...] = dot3(table, halves(spread(slopes, spots, MESH)))
    weights_x, slopes_x = spline(both[3:4, :])
    weights_z, slopes_z = spline(both[5:6, :])
    spots_x = [cells[0] + m for m in range(4)]
    spots_z = [cells[2] + m for m in range(4)]
    along_x = spread(weights_x, spots_x, 24)
    along_z = spread(weights_z, spots_z, ZPAD)
    down_x = spread(slopes_x, spots_x, 24)
    down_z = spread(slopes_z, spots_z, ZPAD)
    for kind, (ax, az) in enumerate(
        ((along_x, along_z), (down_x, along_z), (along_x, down_z))
    ):
        for group, tile in enumerate(planes_of(ax, az)):
            tile_high, tile_low = halves(tile)
            planes[2 * kind, 128 * group : 128 * group + 128, :] = tile_high
            planes[2 * kind + 1, 128 * group : 128 * group + 128, :] = tile_low


def charges_kernel(own, other, weight_y, planes, carry, out, lines):
    charge = jnp.concatenate([own[...], other[...]], axis=1)
    charged = halves(weight_y[...] * charge)
    for group in range(7):
        rows = slice(128 * group, 128 * group + 128)
        line = dot3(charged, (planes[0, rows, :], planes[1, rows, :]), NT)
        kept = line.astype(BF16).astype(F32)
        lines[:, group, :] = kept + dot((line - kept).astype(BF16), carry[...])
    lines[:, 7, :] = jnp.zeros((128, 128), F32)
    out[...] = lines[...].astype(BF16)


def waves_kernel(
    scale_y, received, zh, zl, xh, xl, th, tl, col, row, out, coming, lhs,
):
    for part in range(8):
        lanes = slice(part * 128, part * 128 + 128)
        block = received[part].astype(F32)
        for third in range(3):
            moved = block if third == 0 else pltpu.roll(block, 128 - ZPAD * third, 1)
            coming[third * 128 : third * 128 + 128, lanes] = moved.astype(BF16)
    zed = (zh[...], zl[...])
    lines = dot(coming[...], zed[0]) + dot(coming[...], zed[1])
    total = jnp.zeros((MESH, MESH), F32)
    for third in range(3):
        total += dot3(
            (xh[third], xl[third]), halves(lines[third * 128 : third * 128 + 128, :])
        )
    number = lax.axis_index("gy") * 128 + lax.axis_index("gz") * 16 + lax.axis_index("gx")
    wave = jnp.where(number <= 128, number, number - 128)
    freq_y = wave.astype(F32) / MESH
    square = (col[:, 0:1] + row[0:1, :]) + freq_y * freq_y
    kernel = (col[:, 1:2] * scale_y[number]) * row[1:2, :]
    positive = square > 0.0
    kernel = jnp.where(positive, kernel / jnp.where(positive, square, 1.0), 0.0)
    scaled = halves(total * kernel)
    for third in range(3):
        lhs[third * 128 : third * 128 + 128, :] = dot3(
            halves(dot3((th[third], tl[third]), scaled)), zed, NT
        )
    for part in range(8):
        lanes = slice(part * 128, part * 128 + 128)
        block = lhs[0:128, lanes]
        for third in range(1, 3):
            block += pltpu.roll(lhs[third * 128 : third * 128 + 128, lanes], ZPAD * third, 1)
        out[part] = block


def forces_kernel(weight_y, slope_y, planes, returned, out_own, out_other):
    flat = halves(jnp.concatenate([returned[:, group, :] for group in range(7)], axis=1))

    def level(kind):
        return dot3(flat, (planes[2 * kind], planes[2 * kind + 1]))

    level_0 = level(0)
    along_y = weight_y[...]
    rows = [
        jnp.sum(along_y * level_0, axis=0, keepdims=True),
        jnp.sum(along_y * level(1), axis=0, keepdims=True),
        jnp.sum(slope_y[...] * level_0, axis=0, keepdims=True),
        jnp.sum(along_y * level(2), axis=0, keepdims=True),
        jnp.zeros((4, 256), F32),
    ]
    total = jnp.concatenate(rows, axis=0)
    out_own[...] = total[:, 0:128]
    out_other[...] = total[:, 128:256]


def final_kernel(here, there, charge, base, energy, force):
    total = here[...] + there[...]
    energy[...] = base[...] + 0.5 * charge[...] * total[0:1, :]
    for d in range(3):
        force[:, 128 * d : 128 * d + 128] = -charge[...] * total[1 + d : 2 + d, :]


VMEM = pl.BlockSpec(memory_space=pltpu.VMEM)
SMEM = pl.BlockSpec(memory_space=pltpu.SMEM)


def call(kernel, outs, *args, scratch=(), scalars=(), limit=16):
    specs = [SMEM if i in scalars else VMEM for i in range(len(args))]
    return pl.pallas_call(
        kernel,
        out_shape=[jax.ShapeDtypeStruct(s, d) for s, d in outs],
        in_specs=specs,
        out_specs=[VMEM] * len(outs),
        compiler_params=pltpu.CompilerParams(vmem_limit_bytes=limit << 20),
        scratch_shapes=[pltpu.VMEM(s, d) for s, d in scratch],
    )(*args)


def ring(axis, step):
    count = lax.axis_size(axis)
    return [(i, (i + step) % count) for i in range(count)]


def partner(block):
    return lax.ppermute(block, "gy", [(0, 1), (1, 0)])


def ghosts(blocks):
    width = blocks.shape[1]
    x = blocks.reshape(2, 2, 2, 16, width)
    before = lax.ppermute(x[:, :, 1:], "gz", ring("gz", 1))
    after = lax.ppermute(x[:, :, :1], "gz", ring("gz", -1))
    x = jnp.concatenate([before, x, after], axis=2)
    before = lax.ppermute(x[1:], "gx", ring("gx", 1))
    after = lax.ppermute(x[:1], "gx", ring("gx", -1))
    x = jnp.concatenate([before, x, after], axis=0)
    return x.reshape(512, width), partner(x).reshape(512, width)


def across(blocks):
    return lax.all_to_all(blocks, ("gz", "gx"), split_axis=0, concat_axis=0, tiled=True)


def per_device(
    features, fraction, cell_index, species, octant_rows, neighbours,
    radial_in, radial_out, mix_weight, readout, species_table,
):
    table = constants()
    feats = features[0, 0, 0]
    part = fraction[0, 0, 0]
    cells = cell_index.reshape(1, 3 * ATOMS)
    kinds = species.reshape(1, ATOMS)
    octants = octant_rows[0, 0, 0]
    links = neighbours[0, 0, 0]
    heads = jnp.pad(jnp.transpose(readout), ((0, 6), (0, 0)))

    outgoing, places = call(
        prep_kernel, [((128, 640), BF16), ((8, 128), F32)], feats, part, cells, octants
    )
    near, far = ghosts(outgoing)
    weight_y, slope_y, planes = call(
        static_kernel,
        [((128, 256), F32), ((128, 256), F32), ((6, 896, 256), BF16)],
        places, partner(places), *table["basis_y"],
    )
    feats, outgoing, unit, hidden, rows = call(
        first_kernel,
        [
            ((128, 512), BF16),
            ((128, 512), BF16),
            ((48, 128), F32),
            ((HID, 2048), BF16),
            ((NEIGH, 128), jnp.int32),
        ],
        feats, near, far, part, cells, octants, links, radial_in, radial_out, mix_weight,
        scratch=[
            ((528, 1024), BF16),
            ((512, 2048), BF16),
            ((8, 2048), F32),
            ((512, 2048), F32),
            ((512, 128), BF16),
        ],
        limit=24,
    )
    near, far = ghosts(outgoing)
    feats, charge, base = call(
        second_kernel,
        [((128, 512), BF16), ((1, 128), F32), ((1, 128), F32)],
        feats, near, far, rows, unit, hidden, radial_out, mix_weight, heads, kinds, species_table,
        scalars=(10,),
        scratch=[
            ((512, 1024), BF16),
            ((512, 2048), BF16),
            ((512, 2048), F32),
            ((512, 128), BF16),
        ],
        limit=24,
    )
    (lines,) = call(
        charges_kernel,
        [((128, 8, 128), BF16)],
        charge, partner(charge), weight_y, planes, table["carry"],
        scratch=[((128, 8, 128), F32)],
    )
    received = across(lines).reshape(8, 128, 128)
    (waves,) = call(
        waves_kernel,
        [((8, 128, 128), F32)],
        table["scale_y"], received, *table["basis_z"], *table["basis_x"], *table["basis_xt"],
        table["col"], table["row"],
        scalars=(0,),
        scratch=[((384, 1024), BF16), ((384, 1024), F32)],
    )
    returned = across(waves.reshape(128, 8, 128))
    here, there = call(
        forces_kernel,
        [((8, 128), F32), ((8, 128), F32)],
        weight_y, slope_y, planes, returned,
    )
    energy, force = call(
        final_kernel, [((1, 128), F32), ((1, 384), F32)], here, partner(there), charge, base
    )
    return (
        feats[None, None, None],
        energy.reshape(1, 1, 1, ATOMS),
        force.reshape(1, 1, 1, 3, ATOMS),
    )


def solution(mesh):
    domain = P("gx", "gy", "gz", None, None)
    atoms = P("gx", "gy", "gz", None)
    return jax.shard_map(
        per_device,
        mesh=mesh,
        in_specs=(domain, domain, domain, atoms, domain, domain, P(), P(), P(), P(), P()),
        out_specs=(domain, atoms, domain),
        check_vma=False,
    )
```

```python
import math

import jax
import jax.numpy as jnp
import numpy as np
from jax import lax
from jax.experimental import pallas as pl
from jax.experimental.pallas import tpu as pltpu
from jax.sharding import PartitionSpec as P

C = 128
NB = 8
HID = 64
NEIGH = 16
ENV = 7
MESH = 256
ATOMS = 128
COULOMB = 4.0
EWALD = 0.7
BX, BY, BZ = 16, 128, 32
ZPAD = 40

NODES = (1, 9, 17, 25, 33)

F32 = jnp.float32
BF16 = jnp.bfloat16
NN = (((1,), (0,)), ((), ()))
NT = (((1,), (1,)), ((), ()))
TN = (((0,), (0,)), ((), ()))


def dot(a, b, dims=NN):
    return lax.dot_general(a, b, dims, preferred_element_type=F32)


def halves(x):
    high = x.astype(BF16)
    return high, (x - high.astype(F32)).astype(BF16)


def dot3(a, b, dims=NN):
    return dot(a[0], b[0], dims) + (dot(a[0], b[1], dims) + dot(a[1], b[0], dims))


def np_halves(x):
    x = np.asarray(x, np.float32)
    high = x.astype(BF16)
    return high, (x - high.astype(np.float32)).astype(BF16)


def real_basis():
    rows = np.arange(MESH)
    wave = np.where(rows <= MESH // 2, rows, rows - MESH // 2)
    angle = 2.0 * np.pi * ((wave[:, None] * np.arange(MESH)[None, :]) % MESH) / MESH
    table = np.where((rows <= MESH // 2)[:, None], np.cos(angle), np.sin(angle))
    return wave, table


def constants():
    wave, table = real_basis()
    freq = wave / MESH
    modulus = 9.0 / np.square(2.0 + np.cos(2.0 * np.pi * wave / MESH))
    weight = np.where((wave == 0) | (wave == MESH // 2), 1.0, 2.0)
    factor = np.exp(-(np.pi**2 / EWALD**2) * freq**2) * modulus * weight
    out = {"basis_y": np_halves(table)}
    zed = np.zeros((8, 128, MESH))
    for part in range(8):
        for point in range(35):
            zed[part, point] = table[:, (part * BZ + point - 1) % MESH]
        for spare, node in enumerate(NODES):
            zed[part, 35 + spare] = table[:, (part * BZ + node - 1) % MESH]
    carry = np.zeros((128, 128), np.float32)
    for point in range(35):
        left = min(max((point - 1) // 8, 0), 3)
        share = (point - NODES[left]) / 8.0
        for third in range(3):
            row = ZPAD * third + point
            carry[row, ZPAD * third + 35 + left] = 1.0 - share
            carry[row, ZPAD * third + 36 + left] = share
    out["carry"] = carry.astype(BF16)
    line = np.zeros((128, 128), np.float32)
    move = np.zeros((128, 128), np.float32)
    for third in range(3):
        base = ZPAD * third
        for point in range(35):
            line[base + 35, base + point] = 1.0 - (point - 1) / 32.0
            line[base + 39, base + point] = (point - 1) / 32.0
        move[base + 35, base + 36] = move[base + 39, base + 38] = 1.0
    out["lines"] = np.stack([-line, move - line]).astype(BF16)
    out["basis_z"] = np_halves(zed.reshape(1024, MESH))
    exx = np.zeros((3, MESH, 16, 8))
    for third in range(3):
        for part in range(16):
            for group in range(7):
                point = 3 * group + third
                if point < 19:
                    exx[third, :, part, group] = table[:, (part * BX + point - 1) % MESH]
    exx = exx.reshape(3, MESH, 128)
    out["basis_x"] = np_halves(exx)
    out["basis_xt"] = np_halves(np.swapaxes(exx, 1, 2))
    out["col"] = np.stack([freq**2, factor], axis=1).astype(np.float32)
    row = np.zeros((8, MESH), np.float32)
    row[0], row[1] = freq**2, factor
    out["row"] = row
    out["scale_y"] = (factor * (COULOMB / (math.pi * MESH**3))).astype(np.float32)
    return out


def select_rows(octants):
    slot = lax.broadcasted_iota(jnp.int32, (128, 8), 0)
    group = lax.broadcasted_iota(jnp.int32, (128, 8), 1)
    picker = jnp.where((slot >> 4) == group, 1.0, 0.0).astype(BF16)
    listed = dot(picker, octants[...].astype(F32).astype(BF16))
    spot = lax.broadcasted_iota(jnp.int32, listed.shape, 0) & 15
    entry = lax.broadcasted_iota(jnp.int32, listed.shape, 1)
    wanted = jnp.sum(jnp.where(spot == entry, listed, 0.0), axis=1, keepdims=True)
    lane = lax.broadcasted_iota(jnp.int32, (128, 128), 1).astype(F32)
    return jnp.where(wanted == lane, 1.0, 0.0).astype(BF16)


def cell_rows(cells):
    return [cells[:, 128 * d : 128 * d + 128].astype(F32) for d in range(3)]


def geometry_rows(cells, fraction):
    return jnp.concatenate(
        cell_rows(cells) + [fraction[...].astype(F32), jnp.zeros((122, ATOMS), F32)], axis=0
    )


def prep_kernel(*refs):
    sources, (out, geometry_out), local, signals = refs[:4], refs[4:6], refs[6:10], refs[10]
    copies = [
        pltpu.make_async_copy(source, target, signals.at[i])
        for i, (source, target) in enumerate(zip(sources, local))
    ]
    for copy in copies:
        copy.start()
    for copy in copies:
        copy.wait()
    feats, fraction, cells, octants = local
    chosen = select_rows(octants)
    out[:, :512] = dot(chosen, feats[...]).astype(BF16)
    geometry = geometry_rows(cells, fraction)
    out[:, 512:] = dot(chosen, jnp.transpose(geometry).astype(BF16)).astype(BF16)
    geometry_out[...] = geometry[0:8]


def table_rows(neighbours):
    ghost = neighbours - ATOMS
    outer = (ghost * 4682) >> 16
    spot = ghost - outer * 14
    code = outer
    for bound in (21, 21, 23, 23, 33, 33, 35, 35):
        code = code + (outer >= bound).astype(jnp.int32)
    ex, ey, ez = code >> 4, (code >> 2) & 3, code & 3
    is_ghost = (neighbours >= ATOMS) & (neighbours < 912)
    near = (ey == 1) | (ey == 2)
    half = jnp.where(near, ey - 1, jnp.where(ey == 0, 1, 0))
    base = jnp.where(near, 0, 512)
    row = base + ((ex * 2 + half) * 4 + ez) * 16 + spot
    own = 144 + ((neighbours >> 5) << 6) + (neighbours & 31)
    row = jnp.where(is_ghost, row, jnp.where(neighbours < ATOMS, own, -1))

    def offset(coord, span):
        moved = jnp.where(coord == 3, span, jnp.where(coord == 0, -span, 0))
        return jnp.where(is_ghost, moved, 0).astype(F32)

    return row, (offset(ex, BX), offset(ey, BY), offset(ez, BZ))


def transposed(x):
    return jnp.transpose(x.astype(F32)).astype(BF16)


def fill_table(table, feats, near, far, count, geometry=None):
    own = feats[...]
    if geometry is not None:
        own = jnp.concatenate([own, geometry], axis=1)
    for q in range(4):
        piece = near[128 * q : 128 * q + 128, :]
        if q in (1, 2):
            at = 64 * (q - 1)
            piece = jnp.concatenate(
                [
                    piece[0:16], own[at : at + 32], piece[48:80], own[at + 32 : at + 64],
                    piece[112:128],
                ],
                axis=0,
            )
        table[:, 128 * q : 128 * q + 128] = transposed(piece)[:count]
        piece = far[128 * q : 128 * q + 128, :]
        table[:, 512 + 128 * q : 640 + 128 * q] = transposed(piece)[:count]


def gather_slots(rows, table, gathered, geometry=None):
    for pair in range(NEIGH // 2):
        wanted = jnp.concatenate(
            [rows[2 * pair : 2 * pair + 1, :], rows[2 * pair + 1 : 2 * pair + 2, :]], axis=1
        )
        spots = lax.broadcasted_iota(jnp.int32, (1024, 256), 0)
        one_hot = jnp.where(spots == wanted, 1.0, 0.0).astype(BF16)
        found = dot(table[...], one_hot)
        lanes = slice(pair * 256, pair * 256 + 256)
        gathered[:, lanes] = found[:512].astype(BF16)
        if geometry is not None:
            geometry[:, lanes] = found[512:520]


def silu(x):
    return x * (1.0 / (1.0 + jnp.exp(-x)))


def messages(hidden, radial_out, radial, gathered, unit, message):
    for pair in range(NEIGH // 2):
        lanes = slice(pair * 256, pair * 256 + 256)
        radial[:, lanes] = dot(radial_out, hidden[:, lanes], TN)

    def one_chunk(chunk, carry):
        start = pl.multiple_of(chunk * 32, 32)
        sums = [jnp.zeros((32, 128), F32) for _ in range(4)]
        for slot in range(NEIGH):
            lanes = slice(slot * 128, slot * 128 + 128)
            r = [radial[pl.ds(start + 128 * p, 32), lanes] for p in range(4)]
            s, vx, vy, vz = [
                gathered[pl.ds(start + 128 * p, 32), lanes].astype(F32) for p in range(4)
            ]
            ux = unit[slot : slot + 1, :]
            uy = unit[16 + slot : 17 + slot, :]
            uz = unit[32 + slot : 33 + slot, :]
            sums[0] += r[0] * s + r[1] * (ux * vx + uy * vy + uz * vz)
            scaled = r[2] * s
            sums[1] += ux * scaled + r[3] * vx
            sums[2] += uy * scaled + r[3] * vy
            sums[3] += uz * scaled + r[3] * vz
        for p in range(4):
            message[pl.ds(start + 128 * p, 32), :] = (sums[p] * 0.25).astype(BF16)
        return carry

    lax.fori_loop(0, 4, one_chunk, 0)


def mixed(feats, message, mix_weight, layer, out):
    previous = feats[...].astype(F32)
    scalar = dot(message[0:128, :], mix_weight[layer, 0], TN)
    out[:, 0:128] = (previous[:, 0:128] + silu(scalar)).astype(BF16)
    for d in range(1, 4):
        rows = slice(128 * d, 128 * d + 128)
        moved = dot(message[rows, :], mix_weight[layer, 1], TN)
        out[:, rows] = (previous[:, rows] + moved).astype(BF16)


def first_kernel(
    feats, near, far, fraction, cells, octants, neighbours, radial_in, radial_out, mix_weight,
    new, outgoing, unit, hidden_next, rows_out,
    table, gathered, geometry, radial, message,
):
    own = jnp.transpose(geometry_rows(cells, fraction)).astype(BF16)
    fill_table(table, feats, near, far, 528, own)
    rows, shifts = table_rows(neighbours[...])
    rows_out[...] = rows
    gather_slots(rows, table, gathered, geometry)
    located = jnp.concatenate(cell_rows(cells), axis=0) + fraction[...].astype(F32)
    delta = []
    for d in range(3):
        cell = jnp.concatenate(
            [geometry[d : d + 1, k * 128 : k * 128 + 128] for k in range(NEIGH)], axis=0
        )
        part = jnp.concatenate(
            [geometry[3 + d : 4 + d, k * 128 : k * 128 + 128] for k in range(NEIGH)], axis=0
        )
        delta.append(((cell + shifts[d]) + part) - located[d : d + 1, :])
    length_sq = delta[0] * delta[0] + delta[1] * delta[1] + delta[2] * delta[2]
    distance = jnp.sqrt(length_sq)
    divisor = jnp.sqrt(length_sq + 1.0)
    for d in range(3):
        unit[16 * d : 16 * d + 16, :] = delta[d] / divisor
    envelope = jnp.square(jnp.maximum(1.0 - length_sq / (ENV * ENV), 0.0))
    centres = lax.broadcasted_iota(jnp.int32, (NB, 128), 0).astype(F32)
    basis = []
    for k in range(NEIGH):
        away = distance[k : k + 1, :] - centres
        basis.append(jnp.exp(-(away * away)) * envelope[k : k + 1, :])
    basis = jnp.concatenate(basis, axis=1).astype(BF16)
    hidden = silu(dot(radial_in[0], basis, TN)).astype(BF16)
    hidden_next[...] = silu(dot(radial_in[1], basis, TN)).astype(BF16)
    messages(hidden, radial_out[0], radial, gathered, unit, message)
    mixed(feats, message, mix_weight, 0, new)
    outgoing[...] = dot(select_rows(octants), new[...]).astype(BF16)


def second_kernel(
    feats, near, far, rows, unit, hidden, radial_out, mix_weight, readout, kinds, species_table,
    new, charge, base,
    table, gathered, radial, message,
):
    fill_table(table, feats, near, far, 512)
    gather_slots(rows[...], table, gathered)
    messages(hidden[...], radial_out[1], radial, gathered, unit, message)
    mixed(feats, message, mix_weight, 1, new)
    heads = dot(readout[...], new[:, 0:128], NT)
    second = kinds[...] == 1
    energy = jnp.where(second, species_table[1, 0], species_table[0, 0])
    offset = jnp.where(second, species_table[1, 1], species_table[0, 1])
    base[...] = heads[0:1, :] + energy
    charge[...] = heads[1:2, :] + offset


def spline(t):
    s = 1.0 - t
    weights = [
        s * s * s / 6.0,
        (3.0 * t * t * t - 6.0 * t * t + 4.0) / 6.0,
        (-3.0 * t * t * t + 3.0 * t * t + 3.0 * t + 1.0) / 6.0,
        t * t * t / 6.0,
    ]
    slopes = [
        -0.5 * s * s,
        0.5 * (3.0 * t * t - 4.0 * t),
        0.5 * (-3.0 * t * t + 2.0 * t + 1.0),
        0.5 * t * t,
    ]
    return weights, slopes


def spread(coefficients, spots, count):
    row = lax.broadcasted_iota(jnp.int32, (count, spots[0].shape[1]), 0)
    total = jnp.zeros(row.shape, F32)
    for coefficient, spot in zip(coefficients, spots):
        total = jnp.where(row == spot, coefficient, total)
    return total


def planes_of(along_x, along_z):
    tail = jnp.zeros((8, along_z.shape[1]), F32)
    tiles = []
    for group in range(7):
        parts = [along_z * along_x[3 * group + c : 3 * group + c + 1, :] for c in range(3)]
        tiles.append(jnp.concatenate(parts + [tail], axis=0))
    return tiles


def static_kernel(own, other, high, low, weight_y, slope_y, planes):
    both = jnp.concatenate([own[...], other[...]], axis=1)
    cells = [both[d : d + 1, :].astype(jnp.int32) for d in range(3)]
    half = lax.axis_index("gy")
    lane = lax.broadcasted_iota(jnp.int32, (1, 256), 1)
    domain = jnp.where(lane < 128, half, 1 - half)
    rows = pl.ds(pl.multiple_of(half * 128, 128), 128)
    table = (high[rows, :], low[rows, :])
    weights, slopes = spline(both[4:5, :])
    spots = [(cells[1] + domain * BY + (m - 1)) & (MESH - 1) for m in range(4)]
    weight_y[...] = dot3(table, halves(spread(weights, spots, MESH)))
    slope_y[...] = dot3(table, halves(spread(slopes, spots, MESH)))
    weights_x, slopes_x = spline(both[3:4, :])
    weights_z, slopes_z = spline(both[5:6, :])
    spots_x = [cells[0] + m for m in range(4)]
    spots_z = [cells[2] + m for m in range(4)]
    along_x = spread(weights_x, spots_x, 24)
    along_z = spread(weights_z, spots_z, ZPAD)
    down_x = spread(slopes_x, spots_x, 24)
    down_z = spread(slopes_z, spots_z, ZPAD)
    point = lax.broadcasted_iota(jnp.int32, (ZPAD, 256), 0)
    share = (point - 1).astype(F32) / 32.0

    def with_line(az):
        first = jnp.sum((1.0 - share) * az, axis=0, keepdims=True)
        last = jnp.sum(share * az, axis=0, keepdims=True)
        spare = jnp.where(point < 37, first, jnp.where(point == 37, 0.0, last))
        return jnp.where(point < 35, az, spare)

    along_z, down_z = with_line(along_z), with_line(down_z)
    for kind, (ax, az) in enumerate(
        ((along_x, along_z), (down_x, along_z), (along_x, down_z))
    ):
        for group, tile in enumerate(planes_of(ax, az)):
            tile_high, tile_low = halves(tile)
            planes[2 * kind, 128 * group : 128 * group + 128, :] = tile_high
            planes[2 * kind + 1, 128 * group : 128 * group + 128, :] = tile_low


def charges_kernel(own, other, weight_y, planes, carry, out, lines):
    charge = jnp.concatenate([own[...], other[...]], axis=1)
    charged = halves(weight_y[...] * charge)
    used = lax.broadcasted_iota(jnp.int32, (1, 128), 1) % ZPAD < 35
    for group in range(7):
        rows = slice(128 * group, 128 * group + 128)
        line = jnp.where(used, dot3(charged, (planes[0, rows, :], planes[1, rows, :]), NT), 0.0)
        kept = line.astype(BF16).astype(F32)
        lines[:, group, :] = kept + dot((line - kept).astype(BF16), carry[...])
    lines[:, 7, :] = jnp.zeros((128, 128), F32)
    out[...] = lines[...].astype(BF16)


def waves_kernel(
    scale_y, received, zh, zl, xh, xl, th, tl, col, row, lines, out, coming, lhs,
):
    for part in range(8):
        lanes = slice(part * 128, part * 128 + 128)
        block = received[part].astype(F32)
        for third in range(3):
            moved = block if third == 0 else pltpu.roll(block, 128 - ZPAD * third, 1)
            coming[third * 128 : third * 128 + 128, lanes] = moved.astype(BF16)
    zed = (zh[...], zl[...])
    rows = dot(coming[...], zed[0]) + dot(coming[...], zed[1])
    total = jnp.zeros((MESH, MESH), F32)
    for third in range(3):
        total += dot3(
            (xh[third], xl[third]), halves(rows[third * 128 : third * 128 + 128, :])
        )
    number = lax.axis_index("gy") * 128 + lax.axis_index("gz") * 16 + lax.axis_index("gx")
    wave = jnp.where(number <= 128, number, number - 128)
    freq_y = wave.astype(F32) / MESH
    square = (col[:, 0:1] + row[0:1, :]) + freq_y * freq_y
    kernel = (col[:, 1:2] * scale_y[number]) * row[1:2, :]
    positive = square > 0.0
    kernel = jnp.where(positive, kernel / jnp.where(positive, square, 1.0), 0.0)
    scaled = halves(total * kernel)
    for third in range(3):
        lhs[third * 128 : third * 128 + 128, :] = dot3(
            halves(dot3((th[third], tl[third]), scaled)), zed, NT
        )
    spot = lax.broadcasted_iota(jnp.int32, (1, 128), 1) % ZPAD
    spare = (spot >= 36) & (spot <= 38)
    for part in range(8):
        lanes = slice(part * 128, part * 128 + 128)
        block = lhs[0:128, lanes]
        for third in range(1, 3):
            block += pltpu.roll(lhs[third * 128 : third * 128 + 128, lanes], ZPAD * third, 1)
        high, low = halves(block)
        left = jnp.where(spare, 0.0, block)
        out[part] = (left + dot(high, lines[0]) + dot(low, lines[1])).astype(BF16)


def forces_kernel(weight_y, slope_y, planes, returned, out_own, out_other):
    values = returned[...].astype(F32)
    flat = jnp.concatenate([values[:, group, :] for group in range(7)], axis=1).astype(BF16)

    def level(kind):
        return dot(flat, planes[2 * kind]) + dot(flat, planes[2 * kind + 1])

    level_0 = level(0)
    along_y = weight_y[...]
    rows = [
        jnp.sum(along_y * level_0, axis=0, keepdims=True),
        jnp.sum(along_y * level(1), axis=0, keepdims=True),
        jnp.sum(slope_y[...] * level_0, axis=0, keepdims=True),
        jnp.sum(along_y * level(2), axis=0, keepdims=True),
        jnp.zeros((4, 256), F32),
    ]
    total = jnp.concatenate(rows, axis=0)
    out_own[...] = total[:, 0:128]
    out_other[...] = total[:, 128:256]


def final_kernel(here, there, charge, base, energy, force):
    total = here[...] + there[...]
    energy[...] = base[...] + 0.5 * charge[...] * total[0:1, :]
    for d in range(3):
        force[:, 128 * d : 128 * d + 128] = -charge[...] * total[1 + d : 2 + d, :]


VMEM = pl.BlockSpec(memory_space=pltpu.VMEM)
SMEM = pl.BlockSpec(memory_space=pltpu.SMEM)


def call(kernel, outs, *args, scratch=(), scalars=(), limit=16):
    specs = [SMEM if i in scalars else VMEM for i in range(len(args))]
    return pl.pallas_call(
        kernel,
        out_shape=[jax.ShapeDtypeStruct(s, d) for s, d in outs],
        in_specs=specs,
        out_specs=[VMEM] * len(outs),
        compiler_params=pltpu.CompilerParams(vmem_limit_bytes=limit << 20),
        scratch_shapes=[pltpu.VMEM(s, d) for s, d in scratch],
    )(*args)


def ring(axis, step):
    count = lax.axis_size(axis)
    return [(i, (i + step) % count) for i in range(count)]


def partner(block):
    return lax.ppermute(block, "gy", [(0, 1), (1, 0)])


def ghosts(blocks):
    width = blocks.shape[1]
    x = blocks.reshape(2, 2, 2, 16, width)
    before = lax.ppermute(x[:, :, 1:], "gz", ring("gz", 1))
    after = lax.ppermute(x[:, :, :1], "gz", ring("gz", -1))
    x = jnp.concatenate([before, x, after], axis=2)
    before = lax.ppermute(x[1:], "gx", ring("gx", 1))
    after = lax.ppermute(x[:1], "gx", ring("gx", -1))
    x = jnp.concatenate([before, x, after], axis=0)
    return x.reshape(512, width), partner(x).reshape(512, width)


def across(blocks):
    return lax.all_to_all(blocks, ("gz", "gx"), split_axis=0, concat_axis=0, tiled=True)


def per_device(
    features, fraction, cell_index, species, octant_rows, neighbours,
    radial_in, radial_out, mix_weight, readout, species_table,
):
    table = constants()
    feats = features[0, 0, 0]
    part = fraction[0, 0, 0]
    cells = cell_index.reshape(1, 3 * ATOMS)
    kinds = species.reshape(1, ATOMS)
    octants = octant_rows[0, 0, 0]
    links = neighbours[0, 0, 0]
    heads = jnp.pad(jnp.transpose(readout), ((0, 6), (0, 0)))

    outgoing, places = pl.pallas_call(
        prep_kernel,
        out_shape=[
            jax.ShapeDtypeStruct((128, 640), BF16), jax.ShapeDtypeStruct((8, 128), F32)
        ],
        in_specs=[pl.BlockSpec(memory_space=pltpu.MemorySpace.HBM)] * 4,
        out_specs=[VMEM] * 2,
        scratch_shapes=[
            pltpu.VMEM((128, 512), BF16),
            pltpu.VMEM((3, 128), BF16),
            pltpu.VMEM((1, 384), jnp.int32),
            pltpu.VMEM((8, 14), jnp.int32),
            pltpu.SemaphoreType.DMA((4,)),
        ],
        compiler_params=pltpu.CompilerParams(vmem_limit_bytes=8 << 20),
    )(feats, part, cells, octants)
    near, far = ghosts(outgoing)
    weight_y, slope_y, planes = call(
        static_kernel,
        [((128, 256), F32), ((128, 256), F32), ((6, 896, 256), BF16)],
        places, partner(places), *table["basis_y"],
    )
    feats, outgoing, unit, hidden, rows = call(
        first_kernel,
        [
            ((128, 512), BF16),
            ((128, 512), BF16),
            ((48, 128), F32),
            ((HID, 2048), BF16),
            ((NEIGH, 128), jnp.int32),
        ],
        feats, near, far, part, cells, octants, links, radial_in, radial_out, mix_weight,
        scratch=[
            ((528, 1024), BF16),
            ((512, 2048), BF16),
            ((8, 2048), F32),
            ((512, 2048), F32),
            ((512, 128), BF16),
        ],
        limit=24,
    )
    near, far = ghosts(outgoing)
    feats, charge, base = call(
        second_kernel,
        [((128, 512), BF16), ((1, 128), F32), ((1, 128), F32)],
        feats, near, far, rows, unit, hidden, radial_out, mix_weight, heads, kinds, species_table,
        scalars=(10,),
        scratch=[
            ((512, 1024), BF16),
            ((512, 2048), BF16),
            ((512, 2048), F32),
            ((512, 128), BF16),
        ],
        limit=24,
    )
    (lines,) = call(
        charges_kernel,
        [((128, 8, 128), BF16)],
        charge, partner(charge), weight_y, planes, table["carry"],
        scratch=[((128, 8, 128), F32)],
    )
    received = across(lines).reshape(8, 128, 128)
    (waves,) = call(
        waves_kernel,
        [((8, 128, 128), BF16)],
        table["scale_y"], received, *table["basis_z"], *table["basis_x"], *table["basis_xt"],
        table["col"], table["row"], table["lines"],
        scalars=(0,),
        scratch=[((384, 1024), BF16), ((384, 1024), F32)],
    )
    returned = across(waves.reshape(128, 8, 128))
    here, there = call(
        forces_kernel,
        [((8, 128), F32), ((8, 128), F32)],
        weight_y, slope_y, planes, returned,
    )
    energy, force = call(
        final_kernel, [((1, 128), F32), ((1, 384), F32)], here, partner(there), charge, base
    )
    return (
        feats[None, None, None],
        energy.reshape(1, 1, 1, ATOMS),
        force.reshape(1, 1, 1, 3, ATOMS),
    )


def solution(mesh):
    domain = P("gx", "gy", "gz", None, None)
    atoms = P("gx", "gy", "gz", None)
    return jax.shard_map(
        per_device,
        mesh=mesh,
        in_specs=(domain, domain, domain, atoms, domain, domain, P(), P(), P(), P(), P()),
        out_specs=(domain, atoms, domain),
        check_vma=False,
    )
```

```python
import math

import jax
import jax.numpy as jnp
import numpy as np
from jax import lax
from jax.experimental import pallas as pl
from jax.experimental.pallas import tpu as pltpu
from jax.sharding import PartitionSpec as P


NB = 8
HID = 64
NEIGH = 16
ENV = 7
MESH = 256
ATOMS = 128
COULOMB = 4.0
EWALD = 0.7
BX, BY, BZ = 16, 128, 32
ZPAD = 40

NODES = (1, 9, 17, 25, 33)

F32 = jnp.float32
BF16 = jnp.bfloat16
NN = (((1,), (0,)), ((), ()))
NT = (((1,), (1,)), ((), ()))
TN = (((0,), (0,)), ((), ()))


def dot(a, b, dims=NN):
    return lax.dot_general(a, b, dims, preferred_element_type=F32)


def halves(x):
    high = x.astype(BF16)
    return high, (x - high.astype(F32)).astype(BF16)


def dot3(a, b, dims=NN):
    return dot(a[0], b[0], dims) + (dot(a[0], b[1], dims) + dot(a[1], b[0], dims))


def np_halves(x):
    x = np.asarray(x, np.float32)
    high = x.astype(BF16)
    return high, (x - high.astype(np.float32)).astype(BF16)


def real_basis():
    rows = np.arange(MESH)
    wave = np.where(rows <= MESH // 2, rows, rows - MESH // 2)
    angle = 2.0 * np.pi * ((wave[:, None] * np.arange(MESH)[None, :]) % MESH) / MESH
    table = np.where((rows <= MESH // 2)[:, None], np.cos(angle), np.sin(angle))
    return wave, table


def constants():
    wave, table = real_basis()
    freq = wave / MESH
    modulus = 9.0 / np.square(2.0 + np.cos(2.0 * np.pi * wave / MESH))
    weight = np.where((wave == 0) | (wave == MESH // 2), 1.0, 2.0)
    factor = np.exp(-(np.pi**2 / EWALD**2) * freq**2) * modulus * weight
    out = {"basis_y": np_halves(table)}
    zed = np.zeros((8, 128, MESH))
    for part in range(8):
        for point in range(35):
            zed[part, point] = table[:, (part * BZ + point - 1) % MESH]
        for spare, node in enumerate(NODES):
            zed[part, 35 + spare] = table[:, (part * BZ + node - 1) % MESH]
    carry = np.zeros((128, 128), np.float32)
    for point in range(35):
        left = min(max((point - 1) // 8, 0), 3)
        share = (point - NODES[left]) / 8.0
        for third in range(3):
            row = ZPAD * third + point
            carry[row, ZPAD * third + 35 + left] = 1.0 - share
            carry[row, ZPAD * third + 36 + left] = share
    out["carry"] = carry.astype(BF16)
    line = np.zeros((128, 128), np.float32)
    move = np.zeros((128, 128), np.float32)
    for third in range(3):
        base = ZPAD * third
        for point in range(35):
            line[base + 35, base + point] = 1.0 - (point - 1) / 32.0
            line[base + 39, base + point] = (point - 1) / 32.0
        move[base + 35, base + 36] = move[base + 39, base + 38] = 1.0
    out["lines"] = np.stack([-line, move - line]).astype(BF16)
    out["basis_z"] = np_halves(zed[:, :48].reshape(384, MESH))
    exx = np.zeros((3, MESH, 16, 8))
    for third in range(3):
        for part in range(16):
            for group in range(7):
                point = 3 * group + third
                if point < 19:
                    exx[third, :, part, group] = table[:, (part * BX + point - 1) % MESH]
    exx = exx.reshape(3, MESH, 128)
    out["basis_x"] = np_halves(exx)
    out["col"] = np.stack([freq**2, factor], axis=1).astype(np.float32)
    row = np.zeros((8, MESH), np.float32)
    row[0], row[1] = freq**2, factor
    out["row"] = row
    out["scale_y"] = (factor * (COULOMB / (math.pi * MESH**3))).astype(np.float32)
    return out


def select_rows(octants):
    slot = lax.broadcasted_iota(jnp.int32, (128, 8), 0)
    group = lax.broadcasted_iota(jnp.int32, (128, 8), 1)
    picker = jnp.where((slot >> 4) == group, 1.0, 0.0).astype(BF16)
    listed = dot(picker, octants[...].astype(F32).astype(BF16))
    spot = lax.broadcasted_iota(jnp.int32, listed.shape, 0) & 15
    entry = lax.broadcasted_iota(jnp.int32, listed.shape, 1)
    wanted = jnp.sum(jnp.where(spot == entry, listed, 0.0), axis=1, keepdims=True)
    lane = lax.broadcasted_iota(jnp.int32, (128, 128), 1).astype(F32)
    return jnp.where(wanted == lane, 1.0, 0.0).astype(BF16)


def cell_rows(cells):
    return [cells[:, 128 * d : 128 * d + 128].astype(F32) for d in range(3)]


def geometry_rows(cells, fraction):
    return jnp.concatenate(
        cell_rows(cells) + [fraction[...].astype(F32), jnp.zeros((122, ATOMS), F32)], axis=0
    )


def prep_kernel(*refs):
    sources, (out, geometry_out), local, signals = refs[:4], refs[4:6], refs[6:10], refs[10]
    copies = [
        pltpu.make_async_copy(source, target, signals.at[i])
        for i, (source, target) in enumerate(zip(sources, local))
    ]
    for copy in copies:
        copy.start()
    for copy in copies:
        copy.wait()
    feats, fraction, cells, octants = local
    chosen = select_rows(octants)
    out[:, :512] = dot(chosen, feats[...]).astype(BF16)
    geometry = geometry_rows(cells, fraction)
    out[:, 512:] = dot(chosen, jnp.transpose(geometry).astype(BF16)).astype(BF16)
    geometry_out[...] = geometry[0:8]


def table_rows(neighbours):
    ghost = neighbours - ATOMS
    outer = (ghost * 4682) >> 16
    spot = ghost - outer * 14
    code = outer
    for bound in (21, 21, 23, 23, 33, 33, 35, 35):
        code = code + (outer >= bound).astype(jnp.int32)
    ex, ey, ez = code >> 4, (code >> 2) & 3, code & 3
    is_ghost = (neighbours >= ATOMS) & (neighbours < 912)
    near = (ey == 1) | (ey == 2)
    half = jnp.where(near, ey - 1, jnp.where(ey == 0, 1, 0))
    base = jnp.where(near, 0, 512)
    row = base + ((ex * 2 + half) * 4 + ez) * 16 + spot
    own = 144 + ((neighbours >> 5) << 6) + (neighbours & 31)
    row = jnp.where(is_ghost, row, jnp.where(neighbours < ATOMS, own, -1))

    def offset(coord, span):
        moved = jnp.where(coord == 3, span, jnp.where(coord == 0, -span, 0))
        return jnp.where(is_ghost, moved, 0).astype(F32)

    return row, (offset(ex, BX), offset(ey, BY), offset(ez, BZ))


def transposed(x):
    return jnp.transpose(x.astype(F32)).astype(BF16)


def fill_table(table, feats, near, far, count, geometry=None):
    own = feats[...]
    if geometry is not None:
        own = jnp.concatenate([own, geometry], axis=1)
    for q in range(4):
        piece = near[128 * q : 128 * q + 128, :]
        if q in (1, 2):
            at = 64 * (q - 1)
            piece = jnp.concatenate(
                [
                    piece[0:16], own[at : at + 32], piece[48:80], own[at + 32 : at + 64],
                    piece[112:128],
                ],
                axis=0,
            )
        table[:, 128 * q : 128 * q + 128] = transposed(piece)[:count]
        piece = far[128 * q : 128 * q + 128, :]
        table[:, 512 + 128 * q : 640 + 128 * q] = transposed(piece)[:count]


def gather_slots(rows, table, gathered, geometry=None):
    def one_step(step, carry):
        for pair in (2 * step, 2 * step + 1):
            wanted = jnp.concatenate(
                [rows[pl.ds(2 * pair, 1), :], rows[pl.ds(2 * pair + 1, 1), :]], axis=1
            )
            spots = lax.broadcasted_iota(jnp.int32, (1024, 256), 0)
            one_hot = jnp.where(spots == wanted, 1.0, 0.0).astype(BF16)
            found = dot(table[...], one_hot)
            lanes = pl.ds(pl.multiple_of(pair * 256, 256), 256)
            gathered[:, lanes] = found[:512].astype(BF16)
            if geometry is not None:
                geometry[:, lanes] = found[512:520]
        return carry

    lax.fori_loop(0, NEIGH // 4, one_step, 0)


def silu(x):
    return x * (1.0 / (1.0 + jnp.exp(-x)))


def messages(hidden, radial_out, radial, gathered, unit, message):
    outward = transposed(radial_out)

    def one_step(step, carry):
        lanes = pl.ds(pl.multiple_of(step * 512, 512), 512)
        radial[:, lanes] = dot(outward, hidden[:, lanes])
        return carry

    lax.fori_loop(0, NEIGH // 4, one_step, 0)

    def one_chunk(chunk, carry):
        start = pl.multiple_of(chunk * 32, 32)
        sums = [jnp.zeros((32, 128), F32) for _ in range(4)]
        for slot in range(NEIGH):
            lanes = slice(slot * 128, slot * 128 + 128)
            r = [radial[pl.ds(start + 128 * p, 32), lanes] for p in range(4)]
            s, vx, vy, vz = [
                gathered[pl.ds(start + 128 * p, 32), lanes].astype(F32) for p in range(4)
            ]
            ux = unit[slot : slot + 1, :]
            uy = unit[16 + slot : 17 + slot, :]
            uz = unit[32 + slot : 33 + slot, :]
            sums[0] += r[0] * s + r[1] * (ux * vx + uy * vy + uz * vz)
            scaled = r[2] * s
            sums[1] += ux * scaled + r[3] * vx
            sums[2] += uy * scaled + r[3] * vy
            sums[3] += uz * scaled + r[3] * vz
        for p in range(4):
            message[pl.ds(start + 128 * p, 32), :] = (sums[p] * 0.25).astype(BF16)
        return carry

    lax.fori_loop(0, 4, one_chunk, 0)


def mixed(feats, message, mix_weight, layer, out):
    previous = feats[...].astype(F32)
    scalar = dot(message[0:128, :], mix_weight[layer, 0], TN)
    out[:, 0:128] = (previous[:, 0:128] + silu(scalar)).astype(BF16)
    for d in range(1, 4):
        rows = slice(128 * d, 128 * d + 128)
        moved = dot(message[rows, :], mix_weight[layer, 1], TN)
        out[:, rows] = (previous[:, rows] + moved).astype(BF16)


def first_kernel(
    feats, near, far, fraction, cells, octants, neighbours, radial_in, radial_out, mix_weight,
    new, outgoing, unit, hidden_next, rows_out,
    table, gathered, geometry, radial, message, hidden,
):
    own = jnp.transpose(geometry_rows(cells, fraction)).astype(BF16)
    fill_table(table, feats, near, far, 528, own)
    rows, shifts = table_rows(neighbours[...])
    rows_out[...] = rows
    gather_slots(rows_out, table, gathered, geometry)
    located = jnp.concatenate(cell_rows(cells), axis=0) + fraction[...].astype(F32)
    delta = []
    for d in range(3):
        cell = jnp.concatenate(
            [geometry[d : d + 1, k * 128 : k * 128 + 128] for k in range(NEIGH)], axis=0
        )
        part = jnp.concatenate(
            [geometry[3 + d : 4 + d, k * 128 : k * 128 + 128] for k in range(NEIGH)], axis=0
        )
        delta.append(((cell + shifts[d]) + part) - located[d : d + 1, :])
    length_sq = delta[0] * delta[0] + delta[1] * delta[1] + delta[2] * delta[2]
    distance = jnp.sqrt(length_sq)
    divisor = jnp.sqrt(length_sq + 1.0)
    for d in range(3):
        unit[16 * d : 16 * d + 16, :] = delta[d] / divisor
    envelope = jnp.square(jnp.maximum(1.0 - length_sq / (ENV * ENV), 0.0))
    centres = lax.broadcasted_iota(jnp.int32, (NB, 128), 0).astype(F32)
    basis = []
    for k in range(NEIGH):
        away = distance[k : k + 1, :] - centres
        basis.append(jnp.exp(-(away * away)) * envelope[k : k + 1, :])
    basis = jnp.concatenate(basis, axis=1).astype(BF16)
    hidden[...] = silu(dot(radial_in[0], basis, TN)).astype(BF16)
    hidden_next[...] = silu(dot(radial_in[1], basis, TN)).astype(BF16)
    messages(hidden, radial_out[0], radial, gathered, unit, message)
    mixed(feats, message, mix_weight, 0, new)
    outgoing[...] = dot(select_rows(octants), new[...]).astype(BF16)


def second_kernel(
    feats, near, far, rows, unit, hidden, radial_out, mix_weight, readout, kinds, species_table,
    new, charge, base,
    table, gathered, radial, message,
):
    fill_table(table, feats, near, far, 512)
    gather_slots(rows, table, gathered)
    messages(hidden, radial_out[1], radial, gathered, unit, message)
    mixed(feats, message, mix_weight, 1, new)
    heads = dot(readout[...], new[:, 0:128], NT)
    second = kinds[...] == 1
    energy = jnp.where(second, species_table[1, 0], species_table[0, 0])
    offset = jnp.where(second, species_table[1, 1], species_table[0, 1])
    base[...] = heads[0:1, :] + energy
    charge[...] = heads[1:2, :] + offset


def spline(t):
    s = 1.0 - t
    weights = [
        s * s * s / 6.0,
        (3.0 * t * t * t - 6.0 * t * t + 4.0) / 6.0,
        (-3.0 * t * t * t + 3.0 * t * t + 3.0 * t + 1.0) / 6.0,
        t * t * t / 6.0,
    ]
    slopes = [
        -0.5 * s * s,
        0.5 * (3.0 * t * t - 4.0 * t),
        0.5 * (-3.0 * t * t + 2.0 * t + 1.0),
        0.5 * t * t,
    ]
    return weights, slopes


def spread(coefficients, spots, count):
    row = lax.broadcasted_iota(jnp.int32, (count, spots[0].shape[1]), 0)
    total = jnp.zeros(row.shape, F32)
    for coefficient, spot in zip(coefficients, spots):
        total = jnp.where(row == spot, coefficient, total)
    return total


def planes_of(along_x, along_z):
    tail = jnp.zeros((8, along_z.shape[1]), F32)
    tiles = []
    for group in range(7):
        parts = [along_z * along_x[3 * group + c : 3 * group + c + 1, :] for c in range(3)]
        tiles.append(jnp.concatenate(parts + [tail], axis=0))
    return tiles


def static_kernel(own, other, high, low, weight_y, slope_y, planes):
    both = jnp.concatenate([own[...], other[...]], axis=1)
    cells = [both[d : d + 1, :].astype(jnp.int32) for d in range(3)]
    half = lax.axis_index("gy")
    lane = lax.broadcasted_iota(jnp.int32, (1, 256), 1)
    domain = jnp.where(lane < 128, half, 1 - half)
    rows = pl.ds(pl.multiple_of(half * 128, 128), 128)
    table = (high[rows, :], low[rows, :])
    weights, slopes = spline(both[4:5, :])
    spots = [(cells[1] + domain * BY + (m - 1)) & (MESH - 1) for m in range(4)]
    weight_y[...] = dot3(table, halves(spread(weights, spots, MESH)))
    slope_y[...] = dot3(table, halves(spread(slopes, spots, MESH)))
    weights_x, slopes_x = spline(both[3:4, :])
    weights_z, slopes_z = spline(both[5:6, :])
    spots_x = [cells[0] + m for m in range(4)]
    spots_z = [cells[2] + m for m in range(4)]
    along_x = spread(weights_x, spots_x, 24)
    along_z = spread(weights_z, spots_z, ZPAD)
    down_x = spread(slopes_x, spots_x, 24)
    down_z = spread(slopes_z, spots_z, ZPAD)
    point = lax.broadcasted_iota(jnp.int32, (ZPAD, 256), 0)
    share = (point - 1).astype(F32) / 32.0

    def with_line(az):
        first = jnp.sum((1.0 - share) * az, axis=0, keepdims=True)
        last = jnp.sum(share * az, axis=0, keepdims=True)
        spare = jnp.where(point < 37, first, jnp.where(point == 37, 0.0, last))
        return jnp.where(point < 35, az, spare)

    along_z, down_z = with_line(along_z), with_line(down_z)
    for kind, (ax, az) in enumerate(
        ((along_x, along_z), (down_x, along_z), (along_x, down_z))
    ):
        for group, tile in enumerate(planes_of(ax, az)):
            tile_high, tile_low = halves(tile)
            planes[2 * kind, 128 * group : 128 * group + 128, :] = tile_high
            planes[2 * kind + 1, 128 * group : 128 * group + 128, :] = tile_low


def charges_kernel(own, other, weight_y, planes, carry, out, lines):
    charge = jnp.concatenate([own[...], other[...]], axis=1)
    charged = halves(weight_y[...] * charge)
    used = lax.broadcasted_iota(jnp.int32, (1, 128), 1) % ZPAD < 35
    kept, lost = [], []
    for group in range(7):
        rows = slice(128 * group, 128 * group + 128)
        line = jnp.where(used, dot3(charged, (planes[0, rows, :], planes[1, rows, :]), NT), 0.0)
        kept.append(line.astype(BF16).astype(F32))
        lost.append((line - kept[group]).astype(BF16))
    carried = dot(jnp.concatenate(lost, axis=0), carry[...])
    for group in range(7):
        lines[:, group, :] = kept[group] + carried[128 * group : 128 * group + 128]
    lines[:, 7, :] = jnp.zeros((128, 128), F32)
    out[...] = lines[...].astype(BF16)


def waves_kernel(
    scale_y, received, zh, zl, xh, xl, col, row, lines, out, coming, lhs, zed,
):
    for part in range(8):
        lanes = slice(part * 128, part * 128 + 128)
        block = received[part].astype(F32)
        for third in range(3):
            moved = block if third == 0 else pltpu.roll(block, 128 - ZPAD * third, 1)
            coming[third * 128 : third * 128 + 128, lanes] = moved.astype(BF16)
    for part in range(8):
        for half, source in enumerate((zh, zl)):
            zed[half, part * 128 : part * 128 + 48, :] = source[part * 48 : part * 48 + 48, :]
            zed[half, part * 128 + 48 : part * 128 + 128, :] = jnp.zeros((80, MESH), BF16)
    rows = dot(coming[...], zed[0]) + dot(coming[...], zed[1])
    total = jnp.zeros((MESH, MESH), F32)
    for third in range(3):
        total += dot3(
            (xh[third], xl[third]), halves(rows[third * 128 : third * 128 + 128, :])
        )
    number = lax.axis_index("gy") * 128 + lax.axis_index("gz") * 16 + lax.axis_index("gx")
    wave = jnp.where(number <= 128, number, number - 128)
    freq_y = wave.astype(F32) / MESH
    square = (col[:, 0:1] + row[0:1, :]) + freq_y * freq_y
    kernel = (col[:, 1:2] * scale_y[number]) * row[1:2, :]
    positive = square > 0.0
    kernel = jnp.where(positive, kernel / jnp.where(positive, square, 1.0), 0.0)
    scaled = halves(total * kernel)
    for third in range(3):
        lhs[third * 128 : third * 128 + 128, :] = dot3(
            halves(dot3((xh[third], xl[third]), scaled, TN)), (zed[0], zed[1]), NT
        )
    spot = lax.broadcasted_iota(jnp.int32, (1, 128), 1) % ZPAD
    spare = (spot >= 36) & (spot <= 38)
    for part in range(8):
        lanes = slice(part * 128, part * 128 + 128)
        block = lhs[0:128, lanes]
        for third in range(1, 3):
            block += pltpu.roll(lhs[third * 128 : third * 128 + 128, lanes], ZPAD * third, 1)
        high, low = halves(block)
        left = jnp.where(spare, 0.0, block)
        out[part] = (left + dot(high, lines[0]) + dot(low, lines[1])).astype(BF16)


def forces_kernel(weight_y, slope_y, planes, returned, out_own, out_other):
    values = returned[...].astype(F32)
    flat = jnp.concatenate([values[:, group, :] for group in range(7)], axis=1).astype(BF16)

    def level(kind):
        return dot(flat, planes[2 * kind]) + dot(flat, planes[2 * kind + 1])

    level_0 = level(0)
    along_y = weight_y[...]
    rows = [
        jnp.sum(along_y * level_0, axis=0, keepdims=True),
        jnp.sum(along_y * level(1), axis=0, keepdims=True),
        jnp.sum(slope_y[...] * level_0, axis=0, keepdims=True),
        jnp.sum(along_y * level(2), axis=0, keepdims=True),
        jnp.zeros((4, 256), F32),
    ]
    total = jnp.concatenate(rows, axis=0)
    out_own[...] = total[:, 0:128]
    out_other[...] = total[:, 128:256]


def final_kernel(here, there, charge, base, energy, force):
    total = here[...] + there[...]
    energy[...] = base[...] + 0.5 * charge[...] * total[0:1, :]
    for d in range(3):
        force[:, 128 * d : 128 * d + 128] = -charge[...] * total[1 + d : 2 + d, :]


VMEM = pl.BlockSpec(memory_space=pltpu.VMEM)
SMEM = pl.BlockSpec(memory_space=pltpu.SMEM)


def call(kernel, outs, *args, scratch=(), scalars=(), limit=16):
    specs = [SMEM if i in scalars else VMEM for i in range(len(args))]
    return pl.pallas_call(
        kernel,
        out_shape=[jax.ShapeDtypeStruct(s, d) for s, d in outs],
        in_specs=specs,
        out_specs=[VMEM] * len(outs),
        compiler_params=pltpu.CompilerParams(vmem_limit_bytes=limit << 20),
        scratch_shapes=[pltpu.VMEM(s, d) for s, d in scratch],
    )(*args)


def ring(axis, step):
    count = lax.axis_size(axis)
    return [(i, (i + step) % count) for i in range(count)]


def partner(block):
    return lax.ppermute(block, "gy", [(0, 1), (1, 0)])


def ghosts(blocks):
    width = blocks.shape[1]
    x = blocks.reshape(2, 2, 2, 16, width)
    before = lax.ppermute(x[:, :, 1:], "gz", ring("gz", 1))
    after = lax.ppermute(x[:, :, :1], "gz", ring("gz", -1))
    x = jnp.concatenate([before, x, after], axis=2)
    before = lax.ppermute(x[1:], "gx", ring("gx", 1))
    after = lax.ppermute(x[:1], "gx", ring("gx", -1))
    x = jnp.concatenate([before, x, after], axis=0)
    return x.reshape(512, width), partner(x).reshape(512, width)


def across(blocks):
    return lax.all_to_all(blocks, ("gz", "gx"), split_axis=0, concat_axis=0, tiled=True)


def per_device(
    features, fraction, cell_index, species, octant_rows, neighbours,
    radial_in, radial_out, mix_weight, readout, species_table,
):
    table = constants()
    feats = features[0, 0, 0]
    part = fraction[0, 0, 0]
    cells = cell_index.reshape(1, 3 * ATOMS)
    kinds = species.reshape(1, ATOMS)
    octants = octant_rows[0, 0, 0]
    links = neighbours[0, 0, 0]
    heads = jnp.pad(jnp.transpose(readout), ((0, 6), (0, 0)))

    outgoing, places = pl.pallas_call(
        prep_kernel,
        out_shape=[
            jax.ShapeDtypeStruct((128, 640), BF16), jax.ShapeDtypeStruct((8, 128), F32)
        ],
        in_specs=[pl.BlockSpec(memory_space=pltpu.MemorySpace.HBM)] * 4,
        out_specs=[VMEM] * 2,
        scratch_shapes=[
            pltpu.VMEM((128, 512), BF16),
            pltpu.VMEM((3, 128), BF16),
            pltpu.VMEM((1, 384), jnp.int32),
            pltpu.VMEM((8, 14), jnp.int32),
            pltpu.SemaphoreType.DMA((4,)),
        ],
        compiler_params=pltpu.CompilerParams(vmem_limit_bytes=8 << 20),
    )(*[
        pltpu.with_memory_space_constraint(x, pltpu.MemorySpace.HBM)
        for x in (feats, part, cells, octants)
    ])
    near, far = ghosts(outgoing)
    others = partner(places)
    weight_y, slope_y, planes = call(
        static_kernel,
        [((128, 256), F32), ((128, 256), F32), ((6, 896, 256), BF16)],
        places, others, *table["basis_y"],
    )
    feats, outgoing, unit, hidden, rows = call(
        first_kernel,
        [
            ((128, 512), BF16),
            ((128, 512), BF16),
            ((48, 128), F32),
            ((HID, 2048), BF16),
            ((NEIGH, 128), jnp.int32),
        ],
        feats, near, far, part, cells, octants, links, radial_in, radial_out, mix_weight,
        scratch=[
            ((528, 1024), BF16),
            ((512, 2048), BF16),
            ((8, 2048), F32),
            ((512, 2048), F32),
            ((512, 128), BF16),
            ((HID, 2048), BF16),
        ],
        limit=24,
    )
    near, far = ghosts(outgoing)
    feats, charge, base = call(
        second_kernel,
        [((128, 512), BF16), ((1, 128), F32), ((1, 128), F32)],
        feats, near, far, rows, unit, hidden, radial_out, mix_weight, heads, kinds, species_table,
        scalars=(10,),
        scratch=[
            ((512, 1024), BF16),
            ((512, 2048), BF16),
            ((512, 2048), F32),
            ((512, 128), BF16),
        ],
        limit=24,
    )
    (lines,) = call(
        charges_kernel,
        [((128, 8, 128), BF16)],
        charge, partner(charge), weight_y, planes, table["carry"],
        scratch=[((128, 8, 128), F32)],
    )
    received = across(lines).reshape(8, 128, 128)
    (waves,) = call(
        waves_kernel,
        [((8, 128, 128), BF16)],
        table["scale_y"], received, *table["basis_z"], *table["basis_x"],
        table["col"], table["row"], table["lines"],
        scalars=(0,),
        scratch=[((384, 1024), BF16), ((384, 1024), F32), ((2, 1024, MESH), BF16)],
    )
    returned = across(waves.reshape(128, 8, 128))
    here, there = call(
        forces_kernel,
        [((8, 128), F32), ((8, 128), F32)],
        weight_y, slope_y, planes, returned,
    )
    energy, force = call(
        final_kernel, [((1, 128), F32), ((1, 384), F32)], here, partner(there), charge, base
    )
    return (
        feats[None, None, None],
        energy.reshape(1, 1, 1, ATOMS),
        force.reshape(1, 1, 1, 3, ATOMS),
    )


def solution(mesh):
    domain = P("gx", "gy", "gz", None, None)
    atoms = P("gx", "gy", "gz", None)

    return jax.shard_map(
        per_device,
        mesh=mesh,
        in_specs=(domain, domain, domain, atoms, domain, domain, P(), P(), P(), P(), P()),
        out_specs=(domain, atoms, domain),
        check_vma=False,
    )
```

```python
import math

import jax
import jax.numpy as jnp
import numpy as np
from jax import lax
from jax.experimental import pallas as pl
from jax.experimental.pallas import tpu as pltpu
from jax.sharding import PartitionSpec as P


NB = 8
HID = 64
NEIGH = 16
ENV = 7
MESH = 256
ATOMS = 128
COULOMB = 4.0
EWALD = 0.7
BX, BY, BZ = 16, 128, 32
ZPAD = 40

NODES = (1, 9, 17, 25, 33)

F32 = jnp.float32
BF16 = jnp.bfloat16
NN = (((1,), (0,)), ((), ()))
NT = (((1,), (1,)), ((), ()))
TN = (((0,), (0,)), ((), ()))


def dot(a, b, dims=NN):
    return lax.dot_general(a, b, dims, preferred_element_type=F32)


def halves(x):
    high = x.astype(BF16)
    return high, (x - high.astype(F32)).astype(BF16)


def dot3(a, b, dims=NN):
    return dot(a[0], b[0], dims) + (dot(a[0], b[1], dims) + dot(a[1], b[0], dims))


def np_halves(x):
    x = np.asarray(x, np.float32)
    high = x.astype(BF16)
    return high, (x - high.astype(np.float32)).astype(BF16)


def real_basis():
    rows = np.arange(MESH)
    wave = np.where(rows <= MESH // 2, rows, rows - MESH // 2)
    angle = 2.0 * np.pi * ((wave[:, None] * np.arange(MESH)[None, :]) % MESH) / MESH
    table = np.where((rows <= MESH // 2)[:, None], np.cos(angle), np.sin(angle))
    return wave, table


def constants():
    wave, table = real_basis()
    freq = wave / MESH
    modulus = 9.0 / np.square(2.0 + np.cos(2.0 * np.pi * wave / MESH))
    weight = np.where((wave == 0) | (wave == MESH // 2), 1.0, 2.0)
    factor = np.exp(-(np.pi**2 / EWALD**2) * freq**2) * modulus * weight
    out = {"basis_y": np_halves(table)}
    zed = np.zeros((8, 128, MESH))
    for part in range(8):
        for point in range(35):
            zed[part, point] = table[:, (part * BZ + point - 1) % MESH]
        for spare, node in enumerate(NODES):
            zed[part, 35 + spare] = table[:, (part * BZ + node - 1) % MESH]
    carry = np.zeros((128, 128), np.float32)
    for point in range(35):
        left = min(max((point - 1) // 8, 0), 3)
        share = (point - NODES[left]) / 8.0
        for third in range(3):
            row = ZPAD * third + point
            carry[row, ZPAD * third + 35 + left] = 1.0 - share
            carry[row, ZPAD * third + 36 + left] = share
    out["carry"] = carry.astype(BF16)
    line = np.zeros((128, 128), np.float32)
    move = np.zeros((128, 128), np.float32)
    for third in range(3):
        base = ZPAD * third
        for point in range(35):
            line[base + 35, base + point] = 1.0 - (point - 1) / 32.0
            line[base + 39, base + point] = (point - 1) / 32.0
        move[base + 35, base + 36] = move[base + 39, base + 38] = 1.0
    out["lines"] = np.stack([-line, move - line]).astype(BF16)
    out["basis_z"] = np_halves(zed.reshape(1024, MESH))
    exx = np.zeros((3, MESH, 16, 8))
    for third in range(3):
        for part in range(16):
            for group in range(7):
                point = 3 * group + third
                if point < 19:
                    exx[third, :, part, group] = table[:, (part * BX + point - 1) % MESH]
    exx = exx.reshape(3, MESH, 128)
    out["basis_x"] = np_halves(exx)
    out["basis_xt"] = np_halves(np.swapaxes(exx, 1, 2))
    out["col"] = np.stack([freq**2, factor], axis=1).astype(np.float32)
    row = np.zeros((8, MESH), np.float32)
    row[0], row[1] = freq**2, factor
    out["row"] = row
    out["scale_y"] = (factor * (COULOMB / (math.pi * MESH**3))).astype(np.float32)
    return out


def select_rows(octants):
    slot = lax.broadcasted_iota(jnp.int32, (128, 8), 0)
    group = lax.broadcasted_iota(jnp.int32, (128, 8), 1)
    picker = jnp.where((slot >> 4) == group, 1.0, 0.0).astype(BF16)
    listed = dot(picker, octants[...].astype(F32).astype(BF16))
    spot = lax.broadcasted_iota(jnp.int32, listed.shape, 0) & 15
    entry = lax.broadcasted_iota(jnp.int32, listed.shape, 1)
    wanted = jnp.sum(jnp.where(spot == entry, listed, 0.0), axis=1, keepdims=True)
    lane = lax.broadcasted_iota(jnp.int32, (128, 128), 1).astype(F32)
    return jnp.where(wanted == lane, 1.0, 0.0).astype(BF16)


def cell_rows(cells):
    return [cells[:, 128 * d : 128 * d + 128].astype(F32) for d in range(3)]


def geometry_rows(cells, fraction):
    return jnp.concatenate(
        cell_rows(cells) + [fraction[...].astype(F32), jnp.zeros((122, ATOMS), F32)], axis=0
    )


def prep_kernel(*refs):
    sources, (out, geometry_out), local, signals = refs[:4], refs[4:6], refs[6:10], refs[10]
    copies = [
        pltpu.make_async_copy(source, target, signals.at[i])
        for i, (source, target) in enumerate(zip(sources, local))
    ]
    for copy in copies:
        copy.start()
    for copy in copies:
        copy.wait()
    feats, fraction, cells, octants = local
    chosen = select_rows(octants)
    out[:, :512] = dot(chosen, feats[...]).astype(BF16)
    geometry = geometry_rows(cells, fraction)
    out[:, 512:] = dot(chosen, jnp.transpose(geometry).astype(BF16)).astype(BF16)
    geometry_out[...] = geometry[0:8]


def table_rows(neighbours):
    ghost = neighbours - ATOMS
    outer = (ghost * 4682) >> 16
    spot = ghost - outer * 14
    code = outer
    for bound in (21, 21, 23, 23, 33, 33, 35, 35):
        code = code + (outer >= bound).astype(jnp.int32)
    ex, ey, ez = code >> 4, (code >> 2) & 3, code & 3
    is_ghost = (neighbours >= ATOMS) & (neighbours < 912)
    near = (ey == 1) | (ey == 2)
    half = jnp.where(near, ey - 1, jnp.where(ey == 0, 1, 0))
    base = jnp.where(near, 0, 512)
    row = base + ((ex * 2 + half) * 4 + ez) * 16 + spot
    own = 144 + ((neighbours >> 5) << 6) + (neighbours & 31)
    row = jnp.where(is_ghost, row, jnp.where(neighbours < ATOMS, own, -1))

    def offset(coord, span):
        moved = jnp.where(coord == 3, span, jnp.where(coord == 0, -span, 0))
        return jnp.where(is_ghost, moved, 0).astype(F32)

    return row, (offset(ex, BX), offset(ey, BY), offset(ez, BZ))


def transposed(x):
    return jnp.transpose(x.astype(F32)).astype(BF16)


def fill_table(table, feats, near, far, count, geometry=None):
    own = feats[...]
    if geometry is not None:
        own = jnp.concatenate([own, geometry], axis=1)
    for q in range(4):
        piece = near[128 * q : 128 * q + 128, :]
        if q in (1, 2):
            at = 64 * (q - 1)
            piece = jnp.concatenate(
                [
                    piece[0:16], own[at : at + 32], piece[48:80], own[at + 32 : at + 64],
                    piece[112:128],
                ],
                axis=0,
            )
        table[:, 128 * q : 128 * q + 128] = transposed(piece)[:count]
        piece = far[128 * q : 128 * q + 128, :]
        table[:, 512 + 128 * q : 640 + 128 * q] = transposed(piece)[:count]


def gather_slots(rows, table, gathered, geometry=None):
    for pair in range(NEIGH // 2):
        wanted = jnp.concatenate(
            [rows[2 * pair : 2 * pair + 1, :], rows[2 * pair + 1 : 2 * pair + 2, :]], axis=1
        )
        spots = lax.broadcasted_iota(jnp.int32, (1024, 256), 0)
        one_hot = jnp.where(spots == wanted, 1.0, 0.0).astype(BF16)
        found = dot(table[...], one_hot)
        lanes = slice(pair * 256, pair * 256 + 256)
        gathered[:, lanes] = found[:512].astype(BF16)
        if geometry is not None:
            geometry[:, lanes] = found[512:520]


def silu(x):
    return x * (1.0 / (1.0 + jnp.exp(-x)))


def messages(hidden, radial_out, radial, gathered, unit, message):
    outward = transposed(radial_out)
    for pair in range(NEIGH // 2):
        lanes = slice(pair * 256, pair * 256 + 256)
        radial[:, lanes] = dot(outward, hidden[:, lanes])

    def one_chunk(chunk, carry):
        start = pl.multiple_of(chunk * 32, 32)
        sums = [jnp.zeros((32, 128), F32) for _ in range(4)]
        for slot in range(NEIGH):
            lanes = slice(slot * 128, slot * 128 + 128)
            r = [radial[pl.ds(start + 128 * p, 32), lanes] for p in range(4)]
            s, vx, vy, vz = [
                gathered[pl.ds(start + 128 * p, 32), lanes].astype(F32) for p in range(4)
            ]
            ux = unit[slot : slot + 1, :]
            uy = unit[16 + slot : 17 + slot, :]
            uz = unit[32 + slot : 33 + slot, :]
            sums[0] += r[0] * s + r[1] * (ux * vx + uy * vy + uz * vz)
            scaled = r[2] * s
            sums[1] += ux * scaled + r[3] * vx
            sums[2] += uy * scaled + r[3] * vy
            sums[3] += uz * scaled + r[3] * vz
        for p in range(4):
            message[pl.ds(start + 128 * p, 32), :] = (sums[p] * 0.25).astype(BF16)
        return carry

    lax.fori_loop(0, 4, one_chunk, 0)


def mixed(feats, message, mix_weight, layer, out):
    previous = feats[...].astype(F32)
    scalar = dot(message[0:128, :], mix_weight[layer, 0], TN)
    out[:, 0:128] = (previous[:, 0:128] + silu(scalar)).astype(BF16)
    for d in range(1, 4):
        rows = slice(128 * d, 128 * d + 128)
        moved = dot(message[rows, :], mix_weight[layer, 1], TN)
        out[:, rows] = (previous[:, rows] + moved).astype(BF16)


def first_kernel(
    feats, near, far, fraction, cells, octants, neighbours, radial_in, radial_out, mix_weight,
    new, outgoing, unit, hidden_next, rows_out,
    table, gathered, geometry, radial, message,
):
    own = jnp.transpose(geometry_rows(cells, fraction)).astype(BF16)
    fill_table(table, feats, near, far, 528, own)
    rows, shifts = table_rows(neighbours[...])
    rows_out[...] = rows
    gather_slots(rows, table, gathered, geometry)
    located = jnp.concatenate(cell_rows(cells), axis=0) + fraction[...].astype(F32)
    delta = []
    for d in range(3):
        cell = jnp.concatenate(
            [geometry[d : d + 1, k * 128 : k * 128 + 128] for k in range(NEIGH)], axis=0
        )
        part = jnp.concatenate(
            [geometry[3 + d : 4 + d, k * 128 : k * 128 + 128] for k in range(NEIGH)], axis=0
        )
        delta.append(((cell + shifts[d]) + part) - located[d : d + 1, :])
    length_sq = delta[0] * delta[0] + delta[1] * delta[1] + delta[2] * delta[2]
    distance = jnp.sqrt(length_sq)
    divisor = jnp.sqrt(length_sq + 1.0)
    for d in range(3):
        unit[16 * d : 16 * d + 16, :] = delta[d] / divisor
    envelope = jnp.square(jnp.maximum(1.0 - length_sq / (ENV * ENV), 0.0))
    centres = lax.broadcasted_iota(jnp.int32, (NB, 128), 0).astype(F32)
    basis = []
    for k in range(NEIGH):
        away = distance[k : k + 1, :] - centres
        basis.append(jnp.exp(-(away * away)) * envelope[k : k + 1, :])
    basis = jnp.concatenate(basis, axis=1).astype(BF16)
    hidden = silu(dot(radial_in[0], basis, TN)).astype(BF16)
    hidden_next[...] = silu(dot(radial_in[1], basis, TN)).astype(BF16)
    messages(hidden, radial_out[0], radial, gathered, unit, message)
    mixed(feats, message, mix_weight, 0, new)
    outgoing[...] = dot(select_rows(octants), new[...]).astype(BF16)


def second_kernel(
    feats, near, far, rows, unit, hidden, radial_out, mix_weight, readout, kinds, species_table,
    new, charge, base,
    table, gathered, radial, message,
):
    fill_table(table, feats, near, far, 512)
    gather_slots(rows[...], table, gathered)
    messages(hidden[...], radial_out[1], radial, gathered, unit, message)
    mixed(feats, message, mix_weight, 1, new)
    heads = dot(readout[...], new[:, 0:128], NT)
    second = kinds[...] == 1
    energy = jnp.where(second, species_table[1, 0], species_table[0, 0])
    offset = jnp.where(second, species_table[1, 1], species_table[0, 1])
    base[...] = heads[0:1, :] + energy
    charge[...] = heads[1:2, :] + offset


def spline(t):
    s = 1.0 - t
    weights = [
        s * s * s / 6.0,
        (3.0 * t * t * t - 6.0 * t * t + 4.0) / 6.0,
        (-3.0 * t * t * t + 3.0 * t * t + 3.0 * t + 1.0) / 6.0,
        t * t * t / 6.0,
    ]
    slopes = [
        -0.5 * s * s,
        0.5 * (3.0 * t * t - 4.0 * t),
        0.5 * (-3.0 * t * t + 2.0 * t + 1.0),
        0.5 * t * t,
    ]
    return weights, slopes


def spread(coefficients, spots, count):
    row = lax.broadcasted_iota(jnp.int32, (count, spots[0].shape[1]), 0)
    total = jnp.zeros(row.shape, F32)
    for coefficient, spot in zip(coefficients, spots):
        total = jnp.where(row == spot, coefficient, total)
    return total


def planes_of(along_x, along_z):
    tail = jnp.zeros((8, along_z.shape[1]), F32)
    tiles = []
    for group in range(7):
        parts = [along_z * along_x[3 * group + c : 3 * group + c + 1, :] for c in range(3)]
        tiles.append(jnp.concatenate(parts + [tail], axis=0))
    return tiles


def static_kernel(own, other, high, low, weight_y, slope_y, planes):
    both = jnp.concatenate([own[...], other[...]], axis=1)
    cells = [both[d : d + 1, :].astype(jnp.int32) for d in range(3)]
    half = lax.axis_index("gy")
    lane = lax.broadcasted_iota(jnp.int32, (1, 256), 1)
    domain = jnp.where(lane < 128, half, 1 - half)
    rows = pl.ds(pl.multiple_of(half * 128, 128), 128)
    table = (high[rows, :], low[rows, :])
    weights, slopes = spline(both[4:5, :])
    spots = [(cells[1] + domain * BY + (m - 1)) & (MESH - 1) for m in range(4)]
    weight_y[...] = dot3(table, halves(spread(weights, spots, MESH)))
    slope_y[...] = dot3(table, halves(spread(slopes, spots, MESH)))
    weights_x, slopes_x = spline(both[3:4, :])
    weights_z, slopes_z = spline(both[5:6, :])
    spots_x = [cells[0] + m for m in range(4)]
    spots_z = [cells[2] + m for m in range(4)]
    along_x = spread(weights_x, spots_x, 24)
    along_z = spread(weights_z, spots_z, ZPAD)
    down_x = spread(slopes_x, spots_x, 24)
    down_z = spread(slopes_z, spots_z, ZPAD)
    point = lax.broadcasted_iota(jnp.int32, (ZPAD, 256), 0)
    share = (point - 1).astype(F32) / 32.0

    def with_line(az):
        first = jnp.sum((1.0 - share) * az, axis=0, keepdims=True)
        last = jnp.sum(share * az, axis=0, keepdims=True)
        spare = jnp.where(point < 37, first, jnp.where(point == 37, 0.0, last))
        return jnp.where(point < 35, az, spare)

    along_z, down_z = with_line(along_z), with_line(down_z)
    for kind, (ax, az) in enumerate(
        ((along_x, along_z), (down_x, along_z), (along_x, down_z))
    ):
        for group, tile in enumerate(planes_of(ax, az)):
            tile_high, tile_low = halves(tile)
            planes[2 * kind, 128 * group : 128 * group + 128, :] = tile_high
            planes[2 * kind + 1, 128 * group : 128 * group + 128, :] = tile_low


def charges_kernel(own, other, weight_y, planes, carry, out, lines):
    charge = jnp.concatenate([own[...], other[...]], axis=1)
    charged = halves(weight_y[...] * charge)
    used = lax.broadcasted_iota(jnp.int32, (1, 128), 1) % ZPAD < 35
    kept, lost = [], []
    for group in range(7):
        rows = slice(128 * group, 128 * group + 128)
        line = jnp.where(used, dot3(charged, (planes[0, rows, :], planes[1, rows, :]), NT), 0.0)
        kept.append(line.astype(BF16).astype(F32))
        lost.append((line - kept[group]).astype(BF16))
    carried = dot(jnp.concatenate(lost, axis=0), carry[...])
    for group in range(7):
        lines[:, group, :] = kept[group] + carried[128 * group : 128 * group + 128]
    lines[:, 7, :] = jnp.zeros((128, 128), F32)
    out[...] = lines[...].astype(BF16)


def waves_kernel(
    scale_y, received, zh, zl, xh, xl, th, tl, col, row, lines, out, coming, lhs,
):
    for part in range(8):
        lanes = slice(part * 128, part * 128 + 128)
        block = received[part].astype(F32)
        for third in range(3):
            moved = block if third == 0 else pltpu.roll(block, 128 - ZPAD * third, 1)
            coming[third * 128 : third * 128 + 128, lanes] = moved.astype(BF16)
    zed = (zh[...], zl[...])
    rows = dot(coming[...], zed[0]) + dot(coming[...], zed[1])
    total = jnp.zeros((MESH, MESH), F32)
    for third in range(3):
        total += dot3(
            (xh[third], xl[third]), halves(rows[third * 128 : third * 128 + 128, :])
        )
    number = lax.axis_index("gy") * 128 + lax.axis_index("gz") * 16 + lax.axis_index("gx")
    wave = jnp.where(number <= 128, number, number - 128)
    freq_y = wave.astype(F32) / MESH
    square = (col[:, 0:1] + row[0:1, :]) + freq_y * freq_y
    kernel = (col[:, 1:2] * scale_y[number]) * row[1:2, :]
    positive = square > 0.0
    kernel = jnp.where(positive, kernel / jnp.where(positive, square, 1.0), 0.0)
    scaled = halves(total * kernel)
    for third in range(3):
        lhs[third * 128 : third * 128 + 128, :] = dot3(
            halves(dot3((th[third], tl[third]), scaled)), zed, NT
        )
    spot = lax.broadcasted_iota(jnp.int32, (1, 128), 1) % ZPAD
    spare = (spot >= 36) & (spot <= 38)
    for part in range(8):
        lanes = slice(part * 128, part * 128 + 128)
        block = lhs[0:128, lanes]
        for third in range(1, 3):
            block += pltpu.roll(lhs[third * 128 : third * 128 + 128, lanes], ZPAD * third, 1)
        high, low = halves(block)
        left = jnp.where(spare, 0.0, block)
        out[part] = (left + dot(high, lines[0]) + dot(low, lines[1])).astype(BF16)


def forces_kernel(weight_y, slope_y, planes, returned, out_own, out_other):
    values = returned[...].astype(F32)
    flat = jnp.concatenate([values[:, group, :] for group in range(7)], axis=1).astype(BF16)

    def level(kind):
        return dot(flat, planes[2 * kind]) + dot(flat, planes[2 * kind + 1])

    level_0 = level(0)
    along_y = weight_y[...]
    rows = [
        jnp.sum(along_y * level_0, axis=0, keepdims=True),
        jnp.sum(along_y * level(1), axis=0, keepdims=True),
        jnp.sum(slope_y[...] * level_0, axis=0, keepdims=True),
        jnp.sum(along_y * level(2), axis=0, keepdims=True),
        jnp.zeros((4, 256), F32),
    ]
    total = jnp.concatenate(rows, axis=0)
    out_own[...] = total[:, 0:128]
    out_other[...] = total[:, 128:256]


def final_kernel(here, there, charge, base, energy, force):
    total = here[...] + there[...]
    energy[...] = base[...] + 0.5 * charge[...] * total[0:1, :]
    for d in range(3):
        force[:, 128 * d : 128 * d + 128] = -charge[...] * total[1 + d : 2 + d, :]


VMEM = pl.BlockSpec(memory_space=pltpu.VMEM)
SMEM = pl.BlockSpec(memory_space=pltpu.SMEM)


def call(kernel, outs, *args, scratch=(), scalars=(), limit=16):
    specs = [SMEM if i in scalars else VMEM for i in range(len(args))]
    return pl.pallas_call(
        kernel,
        out_shape=[jax.ShapeDtypeStruct(s, d) for s, d in outs],
        in_specs=specs,
        out_specs=[VMEM] * len(outs),
        compiler_params=pltpu.CompilerParams(vmem_limit_bytes=limit << 20),
        scratch_shapes=[pltpu.VMEM(s, d) for s, d in scratch],
    )(*args)


def ring(axis, step):
    count = lax.axis_size(axis)
    return [(i, (i + step) % count) for i in range(count)]


def partner(block):
    return lax.ppermute(block, "gy", [(0, 1), (1, 0)])


def ghosts(blocks):
    width = blocks.shape[1]
    x = blocks.reshape(2, 2, 2, 16, width)
    before = lax.ppermute(x[:, :, 1:], "gz", ring("gz", 1))
    after = lax.ppermute(x[:, :, :1], "gz", ring("gz", -1))
    x = jnp.concatenate([before, x, after], axis=2)
    before = lax.ppermute(x[1:], "gx", ring("gx", 1))
    after = lax.ppermute(x[:1], "gx", ring("gx", -1))
    x = jnp.concatenate([before, x, after], axis=0)
    return x.reshape(512, width), partner(x).reshape(512, width)


def across(blocks):
    return lax.all_to_all(blocks, ("gz", "gx"), split_axis=0, concat_axis=0, tiled=True)


def per_device(
    features, fraction, cell_index, species, octant_rows, neighbours,
    radial_in, radial_out, mix_weight, readout, species_table,
):
    table = constants()
    feats = features[0, 0, 0]
    part = fraction[0, 0, 0]
    cells = cell_index.reshape(1, 3 * ATOMS)
    kinds = species.reshape(1, ATOMS)
    octants = octant_rows[0, 0, 0]
    links = neighbours[0, 0, 0]
    heads = jnp.pad(jnp.transpose(readout), ((0, 6), (0, 0)))

    outgoing, places = pl.pallas_call(
        prep_kernel,
        out_shape=[
            jax.ShapeDtypeStruct((128, 640), BF16), jax.ShapeDtypeStruct((8, 128), F32)
        ],
        in_specs=[pl.BlockSpec(memory_space=pltpu.MemorySpace.HBM)] * 4,
        out_specs=[VMEM] * 2,
        scratch_shapes=[
            pltpu.VMEM((128, 512), BF16),
            pltpu.VMEM((3, 128), BF16),
            pltpu.VMEM((1, 384), jnp.int32),
            pltpu.VMEM((8, 14), jnp.int32),
            pltpu.SemaphoreType.DMA((4,)),
        ],
        compiler_params=pltpu.CompilerParams(vmem_limit_bytes=8 << 20),
    )(*[
        pltpu.with_memory_space_constraint(x, pltpu.MemorySpace.HBM)
        for x in (feats, part, cells, octants)
    ])
    near, far = ghosts(outgoing)
    others = partner(places)
    weight_y, slope_y, planes = call(
        static_kernel,
        [((128, 256), F32), ((128, 256), F32), ((6, 896, 256), BF16)],
        places, others, *table["basis_y"],
    )
    feats, outgoing, unit, hidden, rows = call(
        first_kernel,
        [
            ((128, 512), BF16),
            ((128, 512), BF16),
            ((48, 128), F32),
            ((HID, 2048), BF16),
            ((NEIGH, 128), jnp.int32),
        ],
        feats, near, far, part, cells, octants, links, radial_in, radial_out, mix_weight,
        scratch=[
            ((528, 1024), BF16),
            ((512, 2048), BF16),
            ((8, 2048), F32),
            ((512, 2048), F32),
            ((512, 128), BF16),
        ],
        limit=24,
    )
    near, far = ghosts(outgoing)
    feats, charge, base = call(
        second_kernel,
        [((128, 512), BF16), ((1, 128), F32), ((1, 128), F32)],
        feats, near, far, rows, unit, hidden, radial_out, mix_weight, heads, kinds, species_table,
        scalars=(10,),
        scratch=[
            ((512, 1024), BF16),
            ((512, 2048), BF16),
            ((512, 2048), F32),
            ((512, 128), BF16),
        ],
        limit=24,
    )
    (lines,) = call(
        charges_kernel,
        [((128, 8, 128), BF16)],
        charge, partner(charge), weight_y, planes, table["carry"],
        scratch=[((128, 8, 128), F32)],
    )
    received = across(lines).reshape(8, 128, 128)
    (waves,) = call(
        waves_kernel,
        [((8, 128, 128), BF16)],
        table["scale_y"], received, *table["basis_z"], *table["basis_x"], *table["basis_xt"],
        table["col"], table["row"], table["lines"],
        scalars=(0,),
        scratch=[((384, 1024), BF16), ((384, 1024), F32)],
    )
    returned = across(waves.reshape(128, 8, 128))
    here, there = call(
        forces_kernel,
        [((8, 128), F32), ((8, 128), F32)],
        weight_y, slope_y, planes, returned,
    )
    energy, force = call(
        final_kernel, [((1, 128), F32), ((1, 384), F32)], here, partner(there), charge, base
    )
    return (
        feats[None, None, None],
        energy.reshape(1, 1, 1, ATOMS),
        force.reshape(1, 1, 1, 3, ATOMS),
    )


def solution(mesh):
    domain = P("gx", "gy", "gz", None, None)
    atoms = P("gx", "gy", "gz", None)

    return jax.shard_map(
        per_device,
        mesh=mesh,
        in_specs=(domain, domain, domain, atoms, domain, domain, P(), P(), P(), P(), P()),
        out_specs=(domain, atoms, domain),
        check_vma=False,
    )
```
